256 devices in a mesh: grp: 8 (over y, core), ep: 32 (over x, z).
Axes of the slice: x: 4, y: 4, z: 8, core: 2. Of those that a mesh axis runs over, the one named last changes fastest.
Arguments:
- d_out: bfloat16 [32768, 2048], P(('grp', 'ep')), may hold values from -12 to 12
- routes: int32 [32768, 2], P(('grp', 'ep')), may hold values from 0 to 7, all different within a row; in each aligned block of 128 rows (0 to 127, 128 to 255, ...) at most 48 rows name the same one
- combine: float32 [32768, 2], P(('grp', 'ep')), may hold values from 0.05 to 1
- live_tokens: int32 [256], P(('grp', 'ep')), may hold values from 1 to 128, as said below
- hidden: bfloat16 [12288, 57344], P('grp', 'ep'), may hold values from -6 to 6
Outputs:
- expert_grad: float32 [2048, 57344], P('grp', 'ep')
The draws below stay inside these ranges and needn't reach their ends.
Inputs may be any that keep to these rules, and one draw needn't show every extreme that they name: `routes`: the two experts of a token differ. Among the 128 rows of one device no expert is named by more than 48 rows, and on some devices one expert is named by exactly 48 rows. `live_tokens`: the live tokens of a device are its first ones; on the last device all 128 are live.
All inputs are finite; a program needn't handle non-finite values.
Results may differ from the reference program's by a relative error of at most 0.0029.
Values may be sent and summed in bfloat16 or wider, within the bound.
A program may use at most 128 MiB of HBM per device.

```python
import math
import jax
import jax.numpy as jnp
import numpy as np
from jax import lax

EXPERTS = 8
DW = 2048
H = 7168
TOK_DEV = 128
CAP = 48
SLOTS_E = 1536
BLOCKS = 256
TOKENS = 32768
N_GRP = 8
N_EP = 32


def draw_live_tokens(key, part):
    index = jnp.arange(BLOCKS, dtype=jnp.int32)
    lowest = TOK_DEV // 4
    base = lowest + (TOK_DEV - lowest) * index // max(BLOCKS - 1, 1)
    jitter = jax.random.randint(jax.random.fold_in(key, 17), (BLOCKS,), 0, TOK_DEV // 8 + 1, dtype=jnp.int32)
    jitter = jnp.where(index == BLOCKS - 1, 0, jitter)
    return jnp.clip(base - jitter, 1, TOK_DEV).astype(jnp.int32)


def block_levels(key, extent, shards, low, top_value):
    def one(dim, blocks):
        draws = jax.random.uniform(jax.random.fold_in(jax.random.fold_in(key, 6), dim), (blocks,), jnp.float32, low / len(shards), top_value / len(shards))
        return jnp.repeat(jnp.exp(draws), extent[dim] // blocks).reshape((-1,) + (1,) * (len(extent) - dim - 1))

    factor_of = one(*shards[0])
    for cut in shards[1:]:
        factor_of = factor_of * one(*cut)
    return factor_of


def assign_block(key, own, number, rows, amount, top, most, skew):
    sequence = jax.random.permutation(key, amount)
    crowded, common = load_shares(amount, rows * top, most, skew, True), load_shares(amount, rows * top, most, skew, False)
    places = jnp.arange(amount)

    def named(sizes, offset_by):
        used = int((sizes > 0).sum())
        fixed = max(1, used // 4)
        moved = fixed + (places - fixed + offset_by * (used - fixed)) % max(1, amount - fixed)
        return jnp.zeros((amount,), jnp.int32).at[sequence[jnp.where(places < fixed, places, moved)]].set(jnp.asarray(sizes, jnp.int32))

    sizes = jnp.where(number % 4 == 0, named(crowded, number // 4), named(common, number - number // 4 - 1))
    mixed = jax.random.permutation(jax.random.fold_in(own, 3), amount)
    donor, taker = mixed[0:amount // 2 * 2:2], mixed[1:amount // 2 * 2:2]
    slack = jnp.minimum(sizes[donor] - 1, most - sizes[taker]) // 2
    slack = jnp.where((donor == sequence[0]) | (taker == sequence[0]) | (sizes[taker] == 0), 0, jnp.maximum(slack, 0))
    moved = jax.random.randint(jax.random.fold_in(own, 4), (amount // 2,), 0, 1 << 20) % (slack + 1)
    sizes = sizes.at[donor].add(-moved).at[taker].add(moved)
    items = jnp.searchsorted(jnp.cumsum(sizes), jnp.arange(rows * top), side="right").astype(jnp.int32)
    table = items.reshape(top, rows).T
    table = table[jax.random.permutation(jax.random.fold_in(own, 1), rows)]
    offset_by = jax.random.randint(jax.random.fold_in(own, 2), (rows, 1), 0, top)
    return jnp.take_along_axis(table, (jnp.arange(top)[None, :] + offset_by) % top, axis=1)


def load_shares(amount, total, bound, skew, full):
    portions = [(1 << 20) // math.isqrt(grade ** skew) + 1 for grade in range(1, amount + 1)]
    largest = bound if full else min(bound, max(-(-total // amount), total * portions[0] // sum(portions)))
    least = 1 if total - largest >= amount - 1 else 0
    given, spare = [largest] + [least] * (amount - 1), total - largest - least * (amount - 1)
    while spare > 0:
        movable = [i for i in range(1, amount) if given[i] < largest] or [i for i in range(1, amount) if given[i] < bound]
        whole, budget = sum([portions[i] for i in movable]), spare
        for i in movable:
            addition = min(bound - given[i], max(1, budget * portions[i] // whole), spare)
            given[i] = given[i] + addition
            spare = spare - addition
    return np.array(given)


def noise(own_key, extent, deviation, limit, shards=(), held_as=jnp.bfloat16):
    gain = block_levels(own_key, extent, shards, -0.22, 0.18) if shards else 1.0
    array = jax.random.normal(own_key, extent, jnp.float32) * deviation * gain
    return jnp.minimum(jnp.maximum(array, -limit), limit).astype(held_as)


def setup_inputs(seed: int = 0) -> dict:
    streams_of = jax.random.split(jax.random.key(seed), 6)
    d_out = noise(streams_of[0], (TOKENS, DW), 2.0, 12.0, ((0, 256),))
    routes_keys = jax.random.split(jax.random.fold_in(streams_of[1], 1), TOKENS // TOK_DEV)
    routes_turns = jax.random.permutation(jax.random.fold_in(streams_of[1], 3), TOKENS // TOK_DEV)
    routes = jax.vmap(lambda own, number: assign_block(jax.random.fold_in(streams_of[1], 2), own, number, TOK_DEV, EXPERTS, 2, CAP, 2))(routes_keys, routes_turns).reshape((TOKENS, 2))
    combine = jnp.clip(jnp.exp(math.log(1.0) - 2.9957323 * jax.random.uniform(streams_of[2], (TOKENS, 2), jnp.float32) ** block_levels(streams_of[2], (TOKENS, 2), ((0, 256),), -0.2, 0.2)), 0.05, 1.0)
    live_tokens = draw_live_tokens(jax.random.fold_in(streams_of[5], 71), 0)
    hidden = noise(streams_of[4], (N_GRP * SLOTS_E, EXPERTS * H), 1.0, 6.0, ((0, 8), (1, 32)))
    return dict(d_out=d_out, routes=routes, combine=combine, live_tokens=live_tokens, hidden=hidden)


def device_slots(d_rows, route_rows, weight_rows, live_count):
    tokens_here = d_rows.shape[0]
    alive = (jnp.arange(tokens_here, dtype=jnp.int32) < live_count).astype(jnp.float32)
    scaled = weight_rows * alive[:, None]
    weighted = (d_rows.astype(jnp.float32)[:, None, :] * scaled[:, :, None]).astype(jnp.bfloat16)
    weighted = weighted.reshape(tokens_here * route_rows.shape[1], d_rows.shape[1])
    flat = route_rows.reshape(-1).astype(jnp.int32)
    chosen = (flat[:, None] == jnp.arange(EXPERTS, dtype=jnp.int32)[None, :]).astype(jnp.int32)
    before = (jnp.cumsum(chosen, axis=0, dtype=jnp.int32) - chosen).astype(jnp.int32)
    position = lax.optimization_barrier(jnp.sum(before * chosen, axis=1, dtype=jnp.int32))
    slot_index = (flat * CAP + position).astype(jnp.int32)
    placing = (jnp.arange(EXPERTS * CAP, dtype=jnp.int32)[:, None] == slot_index[None, :]).astype(jnp.bfloat16)
    buffer = jnp.dot(placing, weighted, preferred_element_type=jnp.float32).astype(jnp.bfloat16)
    alive_pairs = jnp.repeat(alive, route_rows.shape[1])
    counts = lax.optimization_barrier(jnp.sum(chosen.astype(jnp.float32) * alive_pairs[:, None], axis=0))
    return (buffer.reshape(EXPERTS, CAP, d_rows.shape[1]), counts)

def reference(d_out, routes, combine, live_tokens, hidden):
    width = d_out.shape[1]
    group_tokens = N_EP * TOK_DEV

    def group_part(group):
        start = (group * group_tokens).astype(jnp.int32)
        rows = lax.dynamic_slice_in_dim(d_out, start, group_tokens, 0).reshape(N_EP, TOK_DEV, width)
        picks = lax.dynamic_slice_in_dim(routes, start, group_tokens, 0).reshape(N_EP, TOK_DEV, 2)
        weights = lax.dynamic_slice_in_dim(combine, start, group_tokens, 0).reshape(N_EP, TOK_DEV, 2)
        lives = lax.dynamic_slice_in_dim(live_tokens, (group * N_EP).astype(jnp.int32), N_EP, 0)
        buffers, counts = jax.vmap(device_slots)(rows, picks, weights, lives)

        def one_expert(expert):
            slots = lax.dynamic_index_in_dim(buffers, expert, 1, keepdims=False).reshape(N_EP * CAP, width)
            block = lax.dynamic_slice(hidden, ((group * SLOTS_E).astype(jnp.int32), (expert * H).astype(jnp.int32)), (SLOTS_E, H))
            return lax.dot_general(slots, block, (((0,), (0,)), ((), ())), preferred_element_type=jnp.float32)
        partial_value = lax.map(one_expert, jnp.arange(EXPERTS, dtype=jnp.int32))
        return (partial_value, lax.optimization_barrier(jnp.sum(counts, axis=0)))

    def step(carry, group):
        total, count = carry
        partial_value, counts = group_part(group)
        return ((total + partial_value, count + counts), None)
    start = (jnp.zeros((EXPERTS, width, H), jnp.float32), jnp.zeros((EXPERTS,), jnp.float32))
    (total, count), _ = lax.scan(step, start, jnp.arange(N_GRP, dtype=jnp.int32))
    result = total * lax.rsqrt(1.0 + count)[:, None, None]
    return jnp.transpose(result, (1, 0, 2)).reshape(width, EXPERTS * H)
```

```python
import functools

import jax
import jax.numpy as jnp
from jax import lax
from jax.experimental import pallas as pl
from jax.experimental.pallas import tpu as pltpu
from jax.sharding import PartitionSpec as P

EXPERTS = 8
CAP = 48
TOK = 128
CHUNKS = 4
WIDE = 256
HALF = 128
BF = jnp.bfloat16
F32 = jnp.float32


def rcopy(src, dst, ssem, rsem, dev):
    return pltpu.make_async_remote_copy(
        src_ref=src, dst_ref=dst, send_sem=ssem, recv_sem=rsem, device_id=dev,
        device_id_type=pl.DeviceIdType.MESH,
    )


def kernel(
    d_ref, routes_ref, comb_ref, live_ref, hid_ref, out_ref,
    Z, R, S, TR, HB, PB, SC, M, CN, RT, ACC, YS, YV,
    lsem, psem, prx, hsem, hps, hrx, mps, mrx, zs, zx, ms, mx,
    xs, rx, tx, fs, ys, yx, cs, cx,
):
    g = lax.axis_index("grp")
    e = lax.axis_index("ep")
    y, c = g // 2, g % 2
    x, z = e // 8, e % 8
    h = z // 4
    oc = 1 - c

    mate = (y * 2 + oc, e)
    zp = (g, x * 8 + (z + 1) % 8)
    zm = (g, x * 8 + (z + 7) % 8)
    xp = (g, ((x + 1) % 4) * 8 + z)
    xm = (g, ((x + 3) % 4) * 8 + z)
    yp = (((y + 1) % 4) * 2 + c, e)
    ym = (((y + 3) % 4) * 2 + c, e)
    bx1 = (g, (x + 1 - 2 * (x % 2)) * 8 + z)
    bx2 = (g, (3 - x) * 8 + z)
    by1 = ((y + 1 - 2 * (y % 2)) * 2 + c, e)
    by2 = ((3 - y) * 2 + c, e)

    barrier = pltpu.get_barrier_semaphore()
    for dev in (mate, zp, zm, xp, xm, yp, ym):
        pl.semaphore_signal(barrier, inc=1, device_id=dev, device_id_type=pl.DeviceIdType.MESH)

    def column(i, half, core):
        dest = ((y + 2) % 4, None, None, y)[i]
        if dest is None:
            dest = (y + 1) % 4 if half == 0 else (y + 3) % 4
            off = 0 if i == 1 else HALF
        else:
            off = half * HALF
        return pl.ds(pl.multiple_of(WIDE * (2 * dest + core) + off, HALF), HALF)

    mine = pl.ds(pl.multiple_of(c * TOK, TOK), TOK)
    his = pl.ds(pl.multiple_of(oc * TOK, TOK), TOK)

    for i in range(CHUNKS):
        for half in range(2):
            pltpu.make_async_copy(
                d_ref.at[:, column(i, half, c)],
                Z.at[i, z, mine, pl.ds(half * HALF, HALF)],
                lsem.at[i],
            ).start()
    own_rows = pl.ds(pl.multiple_of(c * 1536, 256), 1536)
    mate_rows = pl.ds(pl.multiple_of(oc * 1536, 256), 1536)
    pltpu.make_async_copy(hid_ref, HB.at[own_rows], hsem).start()

    er = lax.broadcasted_iota(jnp.int32, (EXPERTS, TOK), 0)
    tok = lax.broadcasted_iota(jnp.int32, (EXPERTS, TOK), 1)
    first = routes_ref[0:1, :] == er
    second = routes_ref[1:2, :] == er
    chosen = jnp.where(first, 1.0, 0.0) + jnp.where(second, 1.0, 0.0)
    before = (
        lax.broadcasted_iota(jnp.int32, (TOK, TOK), 0)
        < lax.broadcasted_iota(jnp.int32, (TOK, TOK), 1)
    )
    position = jnp.dot(
        chosen.astype(BF), jnp.where(before, 1.0, 0.0).astype(BF), preferred_element_type=F32
    )
    alive = jnp.where(tok < live_ref[0], chosen, 0.0)
    M[z, c, 0:8, :] = jnp.where(alive > 0.0, position, -1.0)
    M[z, c, 8:16, :] = jnp.where(first, comb_ref[0:1, :], 0.0) + jnp.where(
        second, comb_ref[1:2, :], 0.0
    )

    pl.semaphore_wait(barrier, 7)

    rcopy(M.at[z, c], M.at[z, c], mps, mrx, mate).start()
    for i in range(CHUNKS):
        for half in range(2):
            rcopy(
                d_ref.at[:, column(i, half, oc)],
                Z.at[i, z, mine, pl.ds(half * HALF, HALF)],
                psem, prx.at[i], mate,
            ).start()
    hid_copy = rcopy(hid_ref, HB.at[own_rows], hps, hrx, mate)
    hid_copy.start()

    slot_iota = lax.broadcasted_iota(jnp.int32, (CAP, TOK), 0).astype(F32)

    def rows_of(xx, zz):
        return pl.ds(pl.multiple_of((xx * 8 + zz) * CAP, 16), CAP)

    def build_p(b, zz):
        for cc in range(2):
            for k in range(4):
                ex = 2 * ((x + k) % 4) + h
                hit = slot_iota == M[zz, cc, pl.ds(ex, 1), :]
                weight = jnp.where(hit, M[zz, cc, pl.ds(8 + ex, 1), :], 0.0)
                PB[b, cc, CAP * k:CAP * (k + 1), :] = jnp.where(hit, 1.0, 0.0).astype(BF)
                SC[b, cc, CAP * k:CAP * (k + 1), :] = jnp.broadcast_to(
                    jnp.sum(weight, axis=1, keepdims=True), (CAP, TOK)
                )

    def process(i, b, zz):
        @pl.when(i == 0)
        def _():
            build_p(b, zz)

        own = rows_of(x, zz)
        for cc in range(2):
            picked = jnp.dot(
                PB[b, cc], Z[i, zz, cc * TOK:(cc + 1) * TOK, :], preferred_element_type=F32
            )
            scale = SC[b, cc]
            slots = (picked * jnp.concatenate([scale, scale], axis=1)).astype(BF)
            R[i, cc, own, :] = slots[0:CAP]
            for k in range(1, 4):
                S[i, b, k - 1, cc] = slots[CAP * k:CAP * (k + 1)]
        rcopy(S.at[i, b, 0], R.at[i, :, own, :], xs, rx.at[i, 0], xp).start()
        rcopy(S.at[i, b, 2], R.at[i, :, own, :], xs, rx.at[i, 1], xm).start()
        rcopy(S.at[i, b, 1, 0], TR.at[i, b, 0], xs, tx.at[i, b, 0], xp).start()
        rcopy(S.at[i, b, 1, 1], TR.at[i, b, 1], xs, tx.at[i, b, 1], xm).start()

    def forward(i, b, zz):
        for side, dev, src in ((0, xp, (x + 3) % 4), (1, xm, (x + 1) % 4)):
            rcopy(TR.at[i, b, side], TR.at[i, b, side], fs, tx.at[i, b, side], dev).wait_recv()
            rcopy(
                TR.at[i, b, side], R.at[i, side, rows_of(src, zz), :], fs, rx.at[i, 2 + side], dev
            ).start()

    def zsend(i, zz, side, hop, whole):
        dev = (zp, zm)[side]
        ref = Z.at[i, zz] if whole else Z.at[i, zz, pl.ds(side * TOK, TOK)]
        rcopy(ref, ref, zs, zx.at[i, side, hop - 1], dev).start()

    def zwait(i, zz, side, hop, whole):
        dev = (zp, zm)[side]
        ref = Z.at[i, zz] if whole else Z.at[i, zz, pl.ds(side * TOK, TOK)]
        rcopy(ref, ref, zs, zx.at[i, side, hop - 1], dev).wait_recv()

    def msend(zz, side, hop, whole):
        dev = (zp, zm)[side]
        ref = M.at[zz] if whole else M.at[zz, side]
        rcopy(ref, ref, ms, mx.at[side, hop - 1], dev).start()

    def mwait(zz, side, hop, whole):
        dev = (zp, zm)[side]
        ref = M.at[zz] if whole else M.at[zz, side]
        rcopy(ref, ref, ms, mx.at[side, hop - 1], dev).wait_recv()

    def away(hop, side):
        return (z + 8 - hop) % 8 if side == 0 else (z + hop) % 8

    def unit0(i):
        pltpu.make_async_copy(Z.at[i, z, mine], Z.at[i, z, mine], lsem.at[i]).wait()
        rcopy(Z.at[i, z, his], Z.at[i, z, his], psem, prx.at[i], mate).wait_recv()
        for side in range(2):
            zsend(i, z, side, 1, True)
        process(i, 0, z)

    def unit(i, hop):
        for side in range(2):
            block = away(hop, side)

            @pl.when(i == 0)
            def _():
                mwait(block, side, hop, True)
                msend(block, side, hop + 1, hop < 3)

            zwait(i, block, side, hop, True)
            zsend(i, block, side, hop + 1, hop < 3)
        process(i, 2 * hop - 1, away(hop, 0))
        process(i, 2 * hop, away(hop, 1))

    def unit4(i):
        block = away(4, 1)

        @pl.when(i == 0)
        def _():
            for side in range(2):
                mwait(block, side, 4, False)

        for side in range(2):
            zwait(i, block, side, 4, False)
        process(i, 7, block)

    def forward_unit(i, hop):
        if hop == 0:
            forward(i, 0, z)
        elif hop == 4:
            forward(i, 7, away(4, 1))
        else:
            forward(i, 2 * hop - 1, away(hop, 0))
            forward(i, 2 * hop, away(hop, 1))

    def multiply(ch):
        for n in range(2):
            dev = (xp, xm)[n]
            whole = R.at[ch, :, pl.ds(0, 8 * CAP), :]
            rcopy(whole, whole, xs, rx.at[ch, n], dev).wait_recv()
            part = R.at[ch, n, pl.ds(0, 8 * CAP), :]
            rcopy(part, part, fs, rx.at[ch, 2 + n], dev).wait_recv()

        for cc in range(2):
            @pl.loop(0, 6)
            def _(k):
                rows = pl.ds(pl.multiple_of(k * 256, 256), 256)
                cols = pl.ds(pl.multiple_of(cc * 1536 + k * 256, 256), 256)
                RT[:, cols] = R[ch, cc, rows, :].T

        @pl.loop(0, 7)
        def _(n):
            cols = pl.ds(pl.multiple_of(n * 256, 256), 256)
            ACC[:, cols] = jnp.dot(RT[...], HB[:, cols], preferred_element_type=F32)

    def ywait(ch, half):
        ref = YV.at[ch, half]
        rcopy(ref, ref, ys, yx.at[ch, half], (yp, ym)[half]).wait_recv()

    def reduce_send(ch):
        for half in range(2):
            @pl.when(ch == half + 1)
            def _():
                ywait(0, half)

                @pl.loop(0, 7)
                def _(n):
                    cols = pl.ds(pl.multiple_of(n * 256, 256), 256)
                    ACC[half * HALF:(half + 1) * HALF, cols] += YV[0, half, :, cols].astype(F32)

            @pl.loop(0, 7)
            def _(n):
                cols = pl.ds(pl.multiple_of(n * 256, 256), 256)
                YS[ch, half, :, cols] = ACC[half * HALF:(half + 1) * HALF, cols].astype(BF)

            rcopy(YS.at[ch, half], YV.at[ch, half], ys, yx.at[ch, half], (yp, ym)[half]).start()

    def count_send(step):
        dev = (bx1, bx2, by1, by2)[step]
        rcopy(CN.at[0, step], CN.at[1, step], cs, cx.at[step], dev).start()

    def count_wait(step):
        dev = (bx1, bx2, by1, by2)[step]
        rcopy(CN.at[1, step], CN.at[1, step], cs, cx.at[step], dev).wait_recv()
        return CN[0, step] + CN[1, step]

    rcopy(M.at[z, oc], M.at[z, oc], mps, mrx, mate).wait_recv()
    for side in range(2):
        msend(z, side, 1, True)
    unit0(0)

    @pl.loop(0, 5)
    def _(q):
        later = jnp.maximum(q - 1, 0)

        @pl.when(q >= 1)
        def _():
            unit4(later)

        @pl.when(q < 4)
        def _():
            unit(q, 1)
            forward_unit(q, 0)

        @pl.when(q >= 1)
        def _():
            forward_unit(later, 4)

        @pl.when(q == 1)
        def _():
            total = jnp.zeros((EXPERTS, TOK), F32)
            for zz in range(8):
                for cc in range(2):
                    total += jnp.where(M[zz, cc, 0:8, :] >= 0.0, 1.0, 0.0)
            CN[0, 0] = total
            count_send(0)

        for step in range(3):
            @pl.when(q == step + 2)
            def _():
                CN[0, step + 1] = count_wait(step)
                count_send(step + 1)

        @pl.when(q < 4)
        def _():
            unit(q, 2)
            forward_unit(q, 1)
            unit(q, 3)

        @pl.when(q < 3)
        def _():
            unit0(q + 1)

        @pl.when(q < 4)
        def _():
            forward_unit(q, 2)

        @pl.when(q == 1)
        def _():
            pltpu.make_async_copy(hid_ref, HB.at[own_rows], hsem).wait()
            rcopy(hid_ref, HB.at[mate_rows], hps, hrx, mate).wait_recv()

        @pl.when((q >= 1) & (q < 4))
        def _():
            multiply(later)
            reduce_send(later)

        @pl.when(q < 4)
        def _():
            forward_unit(q, 3)

    multiply(3)
    total = count_wait(3)
    picked = jnp.where(er == 2 * x + h, total, 0.0)
    count = jnp.sum(jnp.sum(picked, axis=1, keepdims=True), axis=0, keepdims=True)
    factor = lax.rsqrt(1.0 + count)
    for ch in (1, 2):
        for half in range(2):
            ywait(ch, half)
    for part in range(2):
        rows = slice(part * HALF, (part + 1) * HALF)

        @pl.loop(0, 7)
        def _(n):
            cols = pl.ds(pl.multiple_of(n * 256, 256), 256)
            out_ref[rows, cols] = (
                ACC[rows, cols]
                + YV[part + 1, 0, :, cols].astype(F32)
                + YV[part + 1, 1, :, cols].astype(F32)
            ) * factor

    rcopy(M.at[z, c], M.at[z, c], mps, mrx, mate).wait_send()
    sent = Z.at[:, 0, pl.ds(0, TOK)]
    rcopy(sent, sent, psem, prx.at[0], mate).wait_send()
    hid_copy.wait_send()
    sent = M.at[pl.ds(0, 7)]
    rcopy(sent, sent, ms, mx.at[0, 0], zp).wait_send()
    sent = Z.at[:, pl.ds(0, 7)]
    rcopy(sent, sent, zs, zx.at[0, 0, 0], zp).wait_send()
    rcopy(S, S, xs, rx.at[0, 0], xp).wait_send()
    rcopy(TR, TR, fs, rx.at[0, 0], xp).wait_send()
    rcopy(YS, YS, ys, yx.at[0, 0], yp).wait_send()
    rcopy(CN.at[0], CN.at[0], cs, cx.at[0], bx1).wait_send()


def on_device(d_out, routes, combine, live_tokens, hidden):
    dma = pltpu.SemaphoreType.DMA
    any_spec = pl.BlockSpec(memory_space=pl.ANY)
    vmem = pl.BlockSpec(memory_space=pltpu.VMEM)
    return pl.pallas_call(
        kernel,
        out_shape=jax.ShapeDtypeStruct((WIDE, 1792), F32),
        in_specs=[any_spec, vmem, vmem, pl.BlockSpec(memory_space=pltpu.SMEM), any_spec],
        out_specs=vmem,
        scratch_shapes=[
            pltpu.VMEM((CHUNKS, 8, 2 * TOK, WIDE), BF),
            pltpu.VMEM((CHUNKS, 2, 32 * CAP, WIDE), BF),
            pltpu.VMEM((CHUNKS, 8, 3, 2, CAP, WIDE), BF),
            pltpu.VMEM((CHUNKS, 8, 2, CAP, WIDE), BF),
            pltpu.VMEM((2 * 1536, 1792), BF),
            pltpu.VMEM((8, 2, 4 * CAP, TOK), BF),
            pltpu.VMEM((8, 2, 4 * CAP, TOK), F32),
            pltpu.VMEM((8, 2, 16, TOK), F32),
            pltpu.VMEM((2, 4, EXPERTS, TOK), F32),
            pltpu.VMEM((WIDE, 2 * 1536), BF),
            pltpu.VMEM((WIDE, 1792), F32),
            pltpu.VMEM((3, 2, HALF, 1792), BF),
            pltpu.VMEM((3, 2, HALF, 1792), BF),
            dma((CHUNKS,)), dma, dma((CHUNKS,)), dma, dma, dma, dma, dma,
            dma, dma((CHUNKS, 2, 4)), dma, dma((2, 4)),
            dma, dma((CHUNKS, 4)), dma((CHUNKS, 8, 2)), dma,
            dma, dma((3, 2)), dma, dma((4,)),
        ],
        compiler_params=pltpu.CompilerParams(
            collective_id=0, has_side_effects=True, vmem_limit_bytes=64000000
        ),
    )(d_out, routes.T, combine.T, live_tokens, hidden)


def solution(mesh):
    both = P(("grp", "ep"), None)
    return jax.shard_map(
        on_device, mesh=mesh,
        in_specs=(both, both, both, P(("grp", "ep")), P("grp", "ep")),
        out_specs=P("grp", "ep"), check_vma=False,
    )
```

```python
import functools

import jax
import jax.numpy as jnp
from jax import lax
from jax.experimental import pallas as pl
from jax.experimental.pallas import tpu as pltpu
from jax.sharding import PartitionSpec as P

EXPERTS = 8
CAP = 48
TOK = 128
CHUNKS = 4
WIDE = 256
HALF = 128
KB = 8 * CAP
BF = jnp.bfloat16
F32 = jnp.float32


def rcopy(src, dst, ssem, rsem, dev):
    return pltpu.make_async_remote_copy(
        src_ref=src, dst_ref=dst, send_sem=ssem, recv_sem=rsem, device_id=dev,
        device_id_type=pl.DeviceIdType.MESH,
    )


def kernel(
    d_ref, routes_ref, comb_ref, live_ref, hid_ref, out_ref,
    Z, R, S, HB, PB, SC, M, CN, RT, ACC, YS, YV,
    lsem, psem, prx, hsem, hps, hrx, mps, mrx, zs, zx, ms, mx,
    xs, rx, ys, yx, cs, cx,
):
    g = lax.axis_index("grp")
    e = lax.axis_index("ep")
    y, c = g // 2, g % 2
    x, z = e // 8, e % 8
    h = z // 4
    oc = 1 - c

    mate = (y * 2 + oc, e)
    zp = (g, x * 8 + (z + 1) % 8)
    zm = (g, x * 8 + (z + 7) % 8)
    xp = (g, ((x + 1) % 4) * 8 + z)
    xm = (g, ((x + 3) % 4) * 8 + z)
    xo = (g, ((x + 2) % 4) * 8 + z)
    yp = (((y + 1) % 4) * 2 + c, e)
    ym = (((y + 3) % 4) * 2 + c, e)
    bx1 = (g, (x + 1 - 2 * (x % 2)) * 8 + z)
    bx2 = (g, (3 - x) * 8 + z)
    by1 = ((y + 1 - 2 * (y % 2)) * 2 + c, e)
    by2 = ((3 - y) * 2 + c, e)

    barrier = pltpu.get_barrier_semaphore()
    for dev in (mate, zp, zm, xp, xm, xo, yp, ym):
        pl.semaphore_signal(barrier, inc=1, device_id=dev, device_id_type=pl.DeviceIdType.MESH)

    def column(i, half, core):
        dest = ((y + 2) % 4, None, None, y)[i]
        if dest is None:
            dest = (y + 1) % 4 if half == 0 else (y + 3) % 4
            off = 0 if i == 1 else HALF
        else:
            off = half * HALF
        return pl.ds(pl.multiple_of(WIDE * (2 * dest + core) + off, HALF), HALF)

    mine = pl.ds(pl.multiple_of(c * TOK, TOK), TOK)
    his = pl.ds(pl.multiple_of(oc * TOK, TOK), TOK)

    def source(b):
        hop = (b + 1) // 2
        return (z + 8 - hop) % 8 if b % 2 else (z + hop) % 8

    for i in range(CHUNKS):
        for half in range(2):
            pltpu.make_async_copy(
                d_ref.at[:, column(i, half, c)],
                Z.at[i, z, mine, pl.ds(half * HALF, HALF)],
                lsem.at[i],
            ).start()
    for b in range(8):
        pltpu.make_async_copy(hid_ref.at[:, source(b)], HB.at[b, c], hsem).start()

    er = lax.broadcasted_iota(jnp.int32, (EXPERTS, TOK), 0)
    tok = lax.broadcasted_iota(jnp.int32, (EXPERTS, TOK), 1)
    first = routes_ref[0:1, :] == er
    second = routes_ref[1:2, :] == er
    chosen = jnp.where(first, 1.0, 0.0) + jnp.where(second, 1.0, 0.0)
    before = (
        lax.broadcasted_iota(jnp.int32, (TOK, TOK), 0)
        < lax.broadcasted_iota(jnp.int32, (TOK, TOK), 1)
    )
    position = jnp.dot(
        chosen.astype(BF), jnp.where(before, 1.0, 0.0).astype(BF), preferred_element_type=F32
    )
    alive = jnp.where(tok < live_ref[...], chosen, 0.0)
    M[z, c, 0:8, :] = jnp.where(alive > 0.0, position, -1.0)
    M[z, c, 8:16, :] = jnp.where(first, comb_ref[0:1, :], 0.0) + jnp.where(
        second, comb_ref[1:2, :], 0.0
    )

    pl.semaphore_wait(barrier, 8)

    rcopy(M.at[z, c], M.at[z, c], mps, mrx, mate).start()
    for i in range(CHUNKS):
        for half in range(2):
            rcopy(
                d_ref.at[:, column(i, half, oc)],
                Z.at[i, z, mine, pl.ds(half * HALF, HALF)],
                psem, prx.at[i], mate,
            ).start()
    for b in range(8):
        rcopy(hid_ref.at[:, source(b)], HB.at[b, c], hps, hrx, mate).start()

    slot_iota = lax.broadcasted_iota(jnp.int32, (CAP, TOK), 0).astype(F32)

    def build_p(b, zz):
        for cc in range(2):
            for k in range(4):
                ex = 2 * ((x + k) % 4) + h
                hit = slot_iota == M[zz, cc, pl.ds(ex, 1), :]
                weight = jnp.where(hit, M[zz, cc, pl.ds(8 + ex, 1), :], 0.0)
                PB[b, cc, CAP * k:CAP * (k + 1), :] = jnp.where(hit, 1.0, 0.0).astype(BF)
                SC[b, cc, CAP * k:CAP * (k + 1), :] = jnp.broadcast_to(
                    jnp.sum(weight, axis=1, keepdims=True), (CAP, TOK)
                )

    def wave(b):
        return 0 if b < 5 else 1 if b < 7 else 2

    def process(*units):
        for i, b, zz in units:
            @pl.when(i == 0)
            def _():
                build_p(b, zz)

        for i, b, zz in units:
            for cc in range(2):
                picked = jnp.dot(
                    PB[b, cc], Z[i, zz, cc * TOK:(cc + 1) * TOK, :], preferred_element_type=F32
                )
                scale = SC[b, cc]
                slots = (picked * jnp.concatenate([scale, scale], axis=1)).astype(BF)
                R[i, b, cc, x] = slots[0:CAP]
                for k in range(1, 4):
                    S[i, b, k - 1, cc] = slots[CAP * k:CAP * (k + 1)]
        for i, b, zz in units:
            for k, dev in ((1, xo), (0, xp), (2, xm)):
                rcopy(S.at[i, b, k], R.at[i, b, :, x], xs, rx.at[i, k, wave(b)], dev).start()

    def zsend(i, zz, side, hop, whole):
        dev = (zp, zm)[side]
        ref = Z.at[i, zz] if whole else Z.at[i, zz, pl.ds(side * TOK, TOK)]
        rcopy(ref, ref, zs, zx.at[i, side, hop - 1], dev).start()

    def zwait(i, zz, side, hop, whole):
        dev = (zp, zm)[side]
        ref = Z.at[i, zz] if whole else Z.at[i, zz, pl.ds(side * TOK, TOK)]
        rcopy(ref, ref, zs, zx.at[i, side, hop - 1], dev).wait_recv()

    def msend(zz, side, hop, whole):
        dev = (zp, zm)[side]
        ref = M.at[zz] if whole else M.at[zz, side]
        rcopy(ref, ref, ms, mx.at[side, hop - 1], dev).start()

    def mwait(zz, side, hop, whole):
        dev = (zp, zm)[side]
        ref = M.at[zz] if whole else M.at[zz, side]
        rcopy(ref, ref, ms, mx.at[side, hop - 1], dev).wait_recv()

    def away(hop, side):
        return (z + 8 - hop) % 8 if side == 0 else (z + hop) % 8

    def ready(i):
        pltpu.make_async_copy(Z.at[i, z, mine], Z.at[i, z, mine], lsem.at[i]).wait()
        rcopy(Z.at[i, z, his], Z.at[i, z, his], psem, prx.at[i], mate).wait_recv()

    def z0(i):
        for side in range(2):
            zsend(i, z, side, 1, True)

    def own(i):
        ready(i)
        process((i, 0, z))

    def zhop(i, hop):
        for side in range(2):
            block = away(hop, side)

            @pl.when(i == 0)
            def _():
                mwait(block, side, hop, True)
                msend(block, side, hop + 1, hop < 3)

            zwait(i, block, side, hop, True)
            zsend(i, block, side, hop + 1, hop < 3)

    def z4(i):
        block = away(4, 1)

        @pl.when(i == 0)
        def _():
            for side in range(2):
                mwait(block, side, 4, False)

        for side in range(2):
            zwait(i, block, side, 4, False)

    def both_sides(i, hop):
        process((i, 2 * hop - 1, away(hop, 0)), (i, 2 * hop, away(hop, 1)))

    def arrive(ch, w):
        lo, hi = ((0, 5), (5, 7), (7, 8))[w]
        for k in range(3):
            ref = R.at[ch, lo:hi, :, 0]
            rcopy(ref, ref, xs, rx.at[ch, k, w], (xp, xo, xm)[k]).wait_recv()

    def turn(ch, lo, hi):
        @pl.loop(lo, hi)
        def _(b):
            cols = pl.ds(pl.multiple_of(b * KB, KB), KB)
            RT[:, cols] = R[ch, b].reshape(KB, WIDE).T

    def partial(lo, hi, cols):
        right = HB[lo:hi, :, :, :, cols].reshape((hi - lo) * KB, 256)
        return jnp.dot(RT[:, lo * KB:hi * KB], right, preferred_element_type=F32)

    def column_tiles(body):
        @pl.loop(0, 7)
        def _(n):
            body(pl.ds(pl.multiple_of(n * 256, 256), 256))

    def multiply_first(ch):
        arrive(ch, 0)
        turn(ch, 0, 5)

        @column_tiles
        def _(cols):
            ACC[:, cols] = partial(0, 5, cols)

    def multiply_rest(ch):
        arrive(ch, 1)
        arrive(ch, 2)
        turn(ch, 5, 8)

        @column_tiles
        def _(cols):
            ACC[:, cols] += partial(5, 8, cols)

    def ywait(ch, half):
        ref = YV.at[ch, half]
        rcopy(ref, ref, ys, yx.at[ch, half], (yp, ym)[half]).wait_recv()

    def reduce_send(ch):
        for half in range(2):
            @pl.when(ch == half + 1)
            def _():
                ywait(0, half)

                @pl.loop(0, 7)
                def _(n):
                    cols = pl.ds(pl.multiple_of(n * 256, 256), 256)
                    ACC[half * HALF:(half + 1) * HALF, cols] += YV[0, half, :, cols].astype(F32)

            @pl.loop(0, 7)
            def _(n):
                cols = pl.ds(pl.multiple_of(n * 256, 256), 256)
                YS[ch, half, :, cols] = ACC[half * HALF:(half + 1) * HALF, cols].astype(BF)

            rcopy(YS.at[ch, half], YV.at[ch, half], ys, yx.at[ch, half], (yp, ym)[half]).start()

    def count_send(step):
        dev = (bx1, bx2, by1, by2)[step]
        rcopy(CN.at[0, step], CN.at[1, step], cs, cx.at[step], dev).start()

    def count_wait(step):
        dev = (bx1, bx2, by1, by2)[step]
        rcopy(CN.at[1, step], CN.at[1, step], cs, cx.at[step], dev).wait_recv()
        return CN[0, step] + CN[1, step]

    rcopy(M.at[z, oc], M.at[z, oc], mps, mrx, mate).wait_recv()
    for side in range(2):
        msend(z, side, 1, True)

    ready(0)

    @pl.loop(0, 6)
    def _(q):
        one = jnp.minimum(jnp.maximum(q - 1, 0), 3)
        two = jnp.maximum(q - 2, 0)
        now = jnp.minimum(q, 3)
        young = q < 4
        middle = (q >= 1) & (q < 5)
        old = q >= 2
        done = (q >= 2) & (q < 5)

        pl.when(old)(lambda: z4(two))
        pl.when(middle)(lambda: zhop(one, 2))
        pl.when(young)(lambda: z0(now))

        @pl.when(q == 0)
        def _():
            process((0, 0, z))
            own(1)

        pl.when(old)(lambda: process((two, 7, away(4, 1))))
        pl.when(middle)(lambda: both_sides(one, 2))

        @pl.when(q == 2)
        def _():
            total = jnp.zeros((EXPERTS, TOK), F32)
            for zz in range(8):
                for cc in range(2):
                    total += jnp.where(M[zz, cc, 0:8, :] >= 0.0, 1.0, 0.0)
            CN[0, 0] = total
            count_send(0)
            pltpu.make_async_copy(HB.at[:, c], HB.at[:, c], hsem).wait()
            rcopy(HB.at[:, oc], HB.at[:, oc], hps, hrx, mate).wait_recv()

        for step in range(3):
            @pl.when(q == step + 3)
            def _():
                CN[0, step + 1] = count_wait(step)
                count_send(step + 1)

        pl.when(done)(lambda: multiply_first(two))
        pl.when(middle)(lambda: zhop(one, 3))
        pl.when(young)(lambda: zhop(now, 1))
        pl.when(middle)(lambda: both_sides(one, 3))
        pl.when(young)(lambda: both_sides(now, 1))
        pl.when(q < 2)(lambda: own(jnp.minimum(q + 2, 3)))

        @pl.when(done)
        def _():
            multiply_rest(two)
            reduce_send(two)

    multiply_first(3)
    total = count_wait(3)
    picked = jnp.where(er == 2 * x + h, total, 0.0)
    count = jnp.sum(jnp.sum(picked, axis=1, keepdims=True), axis=0, keepdims=True)
    factor = lax.rsqrt(1.0 + count)
    arrive(3, 1)
    turn(3, 5, 7)
    for ch in (1, 2):
        for half in range(2):
            ywait(ch, half)

    @column_tiles
    def _(cols):
        ACC[:, cols] += partial(5, 7, cols)
        for part in range(2):
            rows = slice(part * HALF, (part + 1) * HALF)
            ACC[rows, cols] += YV[part + 1, 0, :, cols].astype(F32) + YV[
                part + 1, 1, :, cols
            ].astype(F32)

    arrive(3, 2)
    turn(3, 7, 8)

    @column_tiles
    def _(cols):
        out_ref[:, cols] = (ACC[:, cols] + partial(7, 8, cols)) * factor

    rcopy(M.at[z, c], M.at[z, c], mps, mrx, mate).wait_send()
    sent = Z.at[:, 0, pl.ds(0, TOK)]
    rcopy(sent, sent, psem, prx.at[0], mate).wait_send()
    rcopy(HB.at[:, c], HB.at[:, c], hps, hrx, mate).wait_send()
    sent = M.at[pl.ds(0, 7)]
    rcopy(sent, sent, ms, mx.at[0, 0], zp).wait_send()
    sent = Z.at[:, pl.ds(0, 7)]
    rcopy(sent, sent, zs, zx.at[0, 0, 0], zp).wait_send()
    rcopy(S, S, xs, rx.at[0, 0, 0], xp).wait_send()
    rcopy(YS, YS, ys, yx.at[0, 0], yp).wait_send()
    rcopy(CN.at[0], CN.at[0], cs, cx.at[0], bx1).wait_send()


def on_device(d_out, routes, combine, live_tokens, hidden):
    dma = pltpu.SemaphoreType.DMA
    any_spec = pl.BlockSpec(memory_space=pl.ANY)
    vmem = pl.BlockSpec(memory_space=pltpu.VMEM)
    return pl.pallas_call(
        kernel,
        out_shape=jax.ShapeDtypeStruct((WIDE, 1792), F32),
        in_specs=[any_spec, vmem, vmem, vmem, any_spec],
        out_specs=vmem,
        scratch_shapes=[
            pltpu.VMEM((CHUNKS, 8, 2 * TOK, WIDE), BF),
            pltpu.VMEM((CHUNKS, 8, 2, 4, CAP, WIDE), BF),
            pltpu.VMEM((CHUNKS, 8, 3, 2, CAP, WIDE), BF),
            pltpu.VMEM((8, 2, 4, CAP, 1792), BF),
            pltpu.VMEM((8, 2, 4 * CAP, TOK), BF),
            pltpu.VMEM((8, 2, 4 * CAP, TOK), F32),
            pltpu.VMEM((8, 2, 16, TOK), F32),
            pltpu.VMEM((2, 4, EXPERTS, TOK), F32),
            pltpu.VMEM((WIDE, 2 * 1536), BF),
            pltpu.VMEM((WIDE, 1792), F32),
            pltpu.VMEM((3, 2, HALF, 1792), BF),
            pltpu.VMEM((3, 2, HALF, 1792), BF),
            dma((CHUNKS,)), dma, dma((CHUNKS,)), dma, dma, dma, dma, dma,
            dma, dma((CHUNKS, 2, 4)), dma, dma((2, 4)),
            dma, dma((CHUNKS, 3, 3)),
            dma, dma((3, 2)), dma, dma((4,)),
        ],
        compiler_params=pltpu.CompilerParams(
            collective_id=0, has_side_effects=True, vmem_limit_bytes=64000000
        ),
    )(d_out, routes.T, combine.T, live_tokens.reshape(1, 1), hidden.reshape(4, 8, CAP, 1792))


def solution(mesh):
    both = P(("grp", "ep"), None)
    return jax.shard_map(
        on_device, mesh=mesh,
        in_specs=(both, both, both, P(("grp", "ep")), P("grp", "ep")),
        out_specs=P("grp", "ep"), check_vma=False,
    )
```

```python
import functools

import jax
import jax.numpy as jnp
from jax import lax
from jax.experimental import pallas as pl
from jax.experimental.pallas import tpu as pltpu
from jax.sharding import PartitionSpec as P

EXPERTS = 8
CAP = 48
TOK = 128
CHUNKS = 4
WIDE = 256
HALF = 128
KB = 8 * CAP
BF = jnp.bfloat16
F32 = jnp.float32


def rcopy(src, dst, ssem, rsem, dev):
    return pltpu.make_async_remote_copy(
        src_ref=src, dst_ref=dst, send_sem=ssem, recv_sem=rsem, device_id=dev,
        device_id_type=pl.DeviceIdType.MESH,
    )


def kernel(
    d_ref, routes_ref, comb_ref, live_ref, hid_ref, out_ref,
    Z, R, S, HB, PB, SC, M, CN, RT, ACC, YS, YV,
    lsem, psem, prx, hsem, hps, hrx, mps, mrx, zs, zx, ms, mx,
    xs, rx, ys, yx, cs, cx,
):
    g = lax.axis_index("grp")
    e = lax.axis_index("ep")
    y, c = g // 2, g % 2
    x, z = e // 8, e % 8
    h = z // 4
    oc = 1 - c

    mate = (y * 2 + oc, e)
    zp = (g, x * 8 + (z + 1) % 8)
    zm = (g, x * 8 + (z + 7) % 8)
    xp = (g, ((x + 1) % 4) * 8 + z)
    xm = (g, ((x + 3) % 4) * 8 + z)
    xo = (g, ((x + 2) % 4) * 8 + z)
    yp = (((y + 1) % 4) * 2 + c, e)
    ym = (((y + 3) % 4) * 2 + c, e)
    bx1 = (g, (x + 1 - 2 * (x % 2)) * 8 + z)
    bx2 = (g, (3 - x) * 8 + z)
    by1 = ((y + 1 - 2 * (y % 2)) * 2 + c, e)
    by2 = ((3 - y) * 2 + c, e)

    barrier = pltpu.get_barrier_semaphore()
    for dev in (mate, zp, zm, xp, xm, xo, yp, ym):
        pl.semaphore_signal(barrier, inc=1, device_id=dev, device_id_type=pl.DeviceIdType.MESH)

    def column(i, half, core):
        dest = ((y + 2) % 4, None, None, y)[i]
        if dest is None:
            dest = (y + 1) % 4 if half == 0 else (y + 3) % 4
            off = 0 if i == 1 else HALF
        else:
            off = half * HALF
        return pl.ds(pl.multiple_of(WIDE * (2 * dest + core) + off, HALF), HALF)

    mine = pl.ds(pl.multiple_of(c * TOK, TOK), TOK)
    his = pl.ds(pl.multiple_of(oc * TOK, TOK), TOK)

    def source(b):
        hop = (b + 1) // 2
        return (z + 8 - hop) % 8 if b % 2 else (z + hop) % 8

    for i in range(CHUNKS):
        for half in range(2):
            pltpu.make_async_copy(
                d_ref.at[:, column(i, half, c)],
                Z.at[i, z, mine, pl.ds(half * HALF, HALF)],
                lsem.at[i],
            ).start()
    for b in range(8):
        pltpu.make_async_copy(hid_ref.at[:, source(b)], HB.at[b, c], hsem).start()

    er = lax.broadcasted_iota(jnp.int32, (EXPERTS, TOK), 0)
    tok = lax.broadcasted_iota(jnp.int32, (EXPERTS, TOK), 1)
    first = routes_ref[0:1, :] == er
    second = routes_ref[1:2, :] == er
    chosen = jnp.where(first, 1.0, 0.0) + jnp.where(second, 1.0, 0.0)
    before = (
        lax.broadcasted_iota(jnp.int32, (TOK, TOK), 0)
        < lax.broadcasted_iota(jnp.int32, (TOK, TOK), 1)
    )
    position = jnp.dot(
        chosen.astype(BF), jnp.where(before, 1.0, 0.0).astype(BF), preferred_element_type=F32
    )
    alive = jnp.where(tok < live_ref[...], chosen, 0.0)
    M[z, c, 0:8, :] = jnp.where(alive > 0.0, position, -1.0)
    M[z, c, 8:16, :] = jnp.where(first, comb_ref[0:1, :], 0.0) + jnp.where(
        second, comb_ref[1:2, :], 0.0
    )

    pl.semaphore_wait(barrier, 8)

    rcopy(M.at[z, c], M.at[z, c], mps, mrx, mate).start()
    for i in range(CHUNKS):
        for half in range(2):
            rcopy(
                d_ref.at[:, column(i, half, oc)],
                Z.at[i, z, mine, pl.ds(half * HALF, HALF)],
                psem, prx.at[i], mate,
            ).start()
    for b in range(8):
        rcopy(hid_ref.at[:, source(b)], HB.at[b, c], hps, hrx, mate).start()

    slot_iota = lax.broadcasted_iota(jnp.int32, (CAP, TOK), 0).astype(F32)

    def build_p(b, zz):
        for cc in range(2):
            for k in range(4):
                ex = 2 * ((x + k) % 4) + h
                hit = slot_iota == M[zz, cc, pl.ds(ex, 1), :]
                weight = jnp.where(hit, M[zz, cc, pl.ds(8 + ex, 1), :], 0.0)
                PB[b, cc, CAP * k:CAP * (k + 1), :] = jnp.where(hit, 1.0, 0.0).astype(BF)
                SC[b, cc, CAP * k:CAP * (k + 1), :] = jnp.broadcast_to(
                    jnp.sum(weight, axis=1, keepdims=True), (CAP, TOK)
                )

    def wave(b):
        return 0 if b < 5 else 1 if b < 7 else 2

    def process(*units):
        for i, b, zz in units:
            @pl.when(i == 0)
            def _():
                build_p(b, zz)

        for i, b, zz in units:
            for cc in range(2):
                picked = jnp.dot(
                    PB[b, cc], Z[i, zz, cc * TOK:(cc + 1) * TOK, :], preferred_element_type=F32
                )
                scale = SC[b, cc]
                slots = (picked * jnp.concatenate([scale, scale], axis=1)).astype(BF)
                R[i, b, cc, x] = slots[0:CAP]
                for k in range(1, 4):
                    S[i, b, k - 1, cc] = slots[CAP * k:CAP * (k + 1)]
        for i, b, zz in units:
            for k, dev in ((1, xo), (0, xp), (2, xm)):
                rcopy(S.at[i, b, k], R.at[i, b, :, x], xs, rx.at[i, k, wave(b)], dev).start()

    def zsend(i, zz, side, hop, whole):
        dev = (zp, zm)[side]
        ref = Z.at[i, zz] if whole else Z.at[i, zz, pl.ds(side * TOK, TOK)]
        rcopy(ref, ref, zs, zx.at[i, side, hop - 1], dev).start()

    def zwait(i, zz, side, hop, whole):
        dev = (zp, zm)[side]
        ref = Z.at[i, zz] if whole else Z.at[i, zz, pl.ds(side * TOK, TOK)]
        rcopy(ref, ref, zs, zx.at[i, side, hop - 1], dev).wait_recv()

    def msend(zz, side, hop, whole):
        dev = (zp, zm)[side]
        ref = M.at[zz] if whole else M.at[zz, side]
        rcopy(ref, ref, ms, mx.at[side, hop - 1], dev).start()

    def mwait(zz, side, hop, whole):
        dev = (zp, zm)[side]
        ref = M.at[zz] if whole else M.at[zz, side]
        rcopy(ref, ref, ms, mx.at[side, hop - 1], dev).wait_recv()

    def away(hop, side):
        return (z + 8 - hop) % 8 if side == 0 else (z + hop) % 8

    def ready(i):
        pltpu.make_async_copy(Z.at[i, z, mine], Z.at[i, z, mine], lsem.at[i]).wait()
        rcopy(Z.at[i, z, his], Z.at[i, z, his], psem, prx.at[i], mate).wait_recv()

    def z0(i):
        for side in range(2):
            zsend(i, z, side, 1, True)

    def own(i):
        ready(i)
        process((i, 0, z))

    def zhop(i, hop):
        for side in range(2):
            block = away(hop, side)

            @pl.when(i == 0)
            def _():
                mwait(block, side, hop, True)
                msend(block, side, hop + 1, hop < 3)

            zwait(i, block, side, hop, True)
            zsend(i, block, side, hop + 1, hop < 3)

    def z4(i):
        block = away(4, 1)

        @pl.when(i == 0)
        def _():
            for side in range(2):
                mwait(block, side, 4, False)

        for side in range(2):
            zwait(i, block, side, 4, False)

    def both_sides(i, hop):
        process((i, 2 * hop - 1, away(hop, 0)), (i, 2 * hop, away(hop, 1)))

    def arrive(ch, w):
        lo, hi = ((0, 5), (5, 7), (7, 8))[w]
        for k in range(3):
            ref = R.at[ch, lo:hi, :, 0]
            rcopy(ref, ref, xs, rx.at[ch, k, w], (xp, xo, xm)[k]).wait_recv()

    def turn(ch, lo, hi):
        @pl.loop(lo, hi)
        def _(b):
            cols = pl.ds(pl.multiple_of(b * KB, KB), KB)
            RT[:, cols] = R[ch, b].reshape(KB, WIDE).T

    def partial(lo, hi, cols):
        right = HB[lo:hi, :, :, :, cols].reshape((hi - lo) * KB, 256)
        return jnp.dot(RT[:, lo * KB:hi * KB], right, preferred_element_type=F32)

    def column_tiles(body):
        @pl.loop(0, 7)
        def _(n):
            body(pl.ds(pl.multiple_of(n * 256, 256), 256))

    def multiply_first(ch):
        arrive(ch, 0)
        turn(ch, 0, 5)

        @column_tiles
        def _(cols):
            ACC[:, cols] = partial(0, 5, cols)

    def multiply_rest(ch):
        arrive(ch, 1)
        arrive(ch, 2)
        turn(ch, 5, 8)

        @column_tiles
        def _(cols):
            ACC[:, cols] += partial(5, 8, cols)

    def ywait(ch, half):
        ref = YV.at[ch, half]
        rcopy(ref, ref, ys, yx.at[ch, half], (yp, ym)[half]).wait_recv()

    def reduce_send(ch):
        for half in range(2):
            @pl.when(ch == half + 1)
            def _():
                ywait(0, half)

                @pl.loop(0, 7)
                def _(n):
                    cols = pl.ds(pl.multiple_of(n * 256, 256), 256)
                    ACC[half * HALF:(half + 1) * HALF, cols] += YV[0, half, :, cols].astype(F32)

            @pl.loop(0, 7)
            def _(n):
                cols = pl.ds(pl.multiple_of(n * 256, 256), 256)
                YS[ch, half, :, cols] = ACC[half * HALF:(half + 1) * HALF, cols].astype(BF)

            rcopy(YS.at[ch, half], YV.at[ch, half], ys, yx.at[ch, half], (yp, ym)[half]).start()

    def count_send(step):
        dev = (bx1, bx2, by1, by2)[step]
        rcopy(CN.at[0, step], CN.at[1, step], cs, cx.at[step], dev).start()

    def count_wait(step):
        dev = (bx1, bx2, by1, by2)[step]
        rcopy(CN.at[1, step], CN.at[1, step], cs, cx.at[step], dev).wait_recv()
        return CN[0, step] + CN[1, step]

    rcopy(M.at[z, oc], M.at[z, oc], mps, mrx, mate).wait_recv()
    for side in range(2):
        msend(z, side, 1, True)

    ready(0)

    @pl.loop(0, 6)
    def _(q):
        one = jnp.minimum(jnp.maximum(q - 1, 0), 3)
        two = jnp.maximum(q - 2, 0)
        now = jnp.minimum(q, 3)
        young = q < 4
        middle = (q >= 1) & (q < 5)
        old = q >= 2
        done = (q >= 2) & (q < 5)

        pl.when(old)(lambda: z4(two))
        pl.when(middle)(lambda: zhop(one, 2))
        pl.when(young)(lambda: z0(now))

        @pl.when(q == 0)
        def _():
            process((0, 0, z))
            own(1)

        pl.when(old)(lambda: process((two, 7, away(4, 1))))
        pl.when(q == 4)(lambda: both_sides(3, 1))
        pl.when(middle)(lambda: both_sides(one, 2))

        @pl.when(q == 2)
        def _():
            total = jnp.zeros((EXPERTS, TOK), F32)
            for zz in range(8):
                for cc in range(2):
                    total += jnp.where(M[zz, cc, 0:8, :] >= 0.0, 1.0, 0.0)
            CN[0, 0] = total
            count_send(0)
            pltpu.make_async_copy(HB.at[:, c], HB.at[:, c], hsem).wait()
            rcopy(HB.at[:, oc], HB.at[:, oc], hps, hrx, mate).wait_recv()

        for step in range(3):
            @pl.when(q == step + 3)
            def _():
                CN[0, step + 1] = count_wait(step)
                count_send(step + 1)

        pl.when(done)(lambda: multiply_first(two))
        pl.when(middle)(lambda: zhop(one, 3))
        pl.when(young)(lambda: zhop(now, 1))
        pl.when(middle)(lambda: both_sides(one, 3))
        pl.when(q < 3)(lambda: both_sides(now, 1))

        @pl.when(q == 0)
        def _():
            own(2)
            ready(3)

        @pl.when(q == 4)
        def _():
            process((3, 0, z))


        @pl.when(done)
        def _():
            multiply_rest(two)
            reduce_send(two)

    multiply_first(3)
    total = count_wait(3)
    picked = jnp.where(er == 2 * x + h, total, 0.0)
    count = jnp.sum(jnp.sum(picked, axis=1, keepdims=True), axis=0, keepdims=True)
    factor = lax.rsqrt(1.0 + count)
    arrive(3, 1)
    turn(3, 5, 7)
    for ch in (1, 2):
        for half in range(2):
            ywait(ch, half)

    @column_tiles
    def _(cols):
        ACC[:, cols] += partial(5, 7, cols)
        for part in range(2):
            rows = slice(part * HALF, (part + 1) * HALF)
            ACC[rows, cols] += YV[part + 1, 0, :, cols].astype(F32) + YV[
                part + 1, 1, :, cols
            ].astype(F32)

    arrive(3, 2)
    turn(3, 7, 8)

    @column_tiles
    def _(cols):
        out_ref[:, cols] = (ACC[:, cols] + partial(7, 8, cols)) * factor

    rcopy(M.at[z, c], M.at[z, c], mps, mrx, mate).wait_send()
    sent = Z.at[:, 0, pl.ds(0, TOK)]
    rcopy(sent, sent, psem, prx.at[0], mate).wait_send()
    rcopy(HB.at[:, c], HB.at[:, c], hps, hrx, mate).wait_send()
    sent = M.at[pl.ds(0, 7)]
    rcopy(sent, sent, ms, mx.at[0, 0], zp).wait_send()
    sent = Z.at[:, pl.ds(0, 7)]
    rcopy(sent, sent, zs, zx.at[0, 0, 0], zp).wait_send()
    rcopy(S, S, xs, rx.at[0, 0, 0], xp).wait_send()
    rcopy(YS, YS, ys, yx.at[0, 0], yp).wait_send()
    rcopy(CN.at[0], CN.at[0], cs, cx.at[0], bx1).wait_send()


def on_device(d_out, routes, combine, live_tokens, hidden):
    dma = pltpu.SemaphoreType.DMA
    any_spec = pl.BlockSpec(memory_space=pl.ANY)
    vmem = pl.BlockSpec(memory_space=pltpu.VMEM)
    return pl.pallas_call(
        kernel,
        out_shape=jax.ShapeDtypeStruct((WIDE, 1792), F32),
        in_specs=[any_spec, vmem, vmem, vmem, any_spec],
        out_specs=vmem,
        scratch_shapes=[
            pltpu.VMEM((CHUNKS, 8, 2 * TOK, WIDE), BF),
            pltpu.VMEM((CHUNKS, 8, 2, 4, CAP, WIDE), BF),
            pltpu.VMEM((CHUNKS, 8, 3, 2, CAP, WIDE), BF),
            pltpu.VMEM((8, 2, 4, CAP, 1792), BF),
            pltpu.VMEM((8, 2, 4 * CAP, TOK), BF),
            pltpu.VMEM((8, 2, 4 * CAP, TOK), F32),
            pltpu.VMEM((8, 2, 16, TOK), F32),
            pltpu.VMEM((2, 4, EXPERTS, TOK), F32),
            pltpu.VMEM((WIDE, 2 * 1536), BF),
            pltpu.VMEM((WIDE, 1792), F32),
            pltpu.VMEM((3, 2, HALF, 1792), BF),
            pltpu.VMEM((3, 2, HALF, 1792), BF),
            dma((CHUNKS,)), dma, dma((CHUNKS,)), dma, dma, dma, dma, dma,
            dma, dma((CHUNKS, 2, 4)), dma, dma((2, 4)),
            dma, dma((CHUNKS, 3, 3)),
            dma, dma((3, 2)), dma, dma((4,)),
        ],
        compiler_params=pltpu.CompilerParams(
            collective_id=0, has_side_effects=True, vmem_limit_bytes=54000000
        ),
    )(d_out, routes.T, combine.T, live_tokens.reshape(1, 1), hidden.reshape(4, 8, CAP, 1792))


def solution(mesh):
    both = P(("grp", "ep"), None)
    return jax.shard_map(
        on_device, mesh=mesh,
        in_specs=(both, both, both, P(("grp", "ep")), P("grp", "ep")),
        out_specs=P("grp", "ep"), check_vma=False,
    )
```

```python
import functools

import jax
import jax.numpy as jnp
from jax import lax
from jax.experimental import pallas as pl
from jax.experimental.pallas import tpu as pltpu
from jax.sharding import PartitionSpec as P

EXPERTS = 8
CAP = 48
TOK = 128
CHUNKS = 4
WIDE = 256
HALF = 128
PLAN = (
    "z00", "p00", "r1", "p10", "r3",
    "z01", "p01", "r2", "p20",
    "z02", "z10", "p02",
    "z03", "z11", "p03", "p11",
    "z04", "z12", "z20", "p04", "p12", "c0", "h", "f0",
    "z13", "z21", "p13", "p21", "l0",
    "z14", "z22", "z30", "p14", "p22", "c1", "f1",
    "z23", "z31", "p23", "p30", "c2", "l1",
    "z24", "z32", "p24", "p31", "p32", "c3", "f2",
    "z33", "p33", "l2",
    "z34", "p34",
)
KB = 8 * CAP
BF = jnp.bfloat16
F32 = jnp.float32


def rcopy(src, dst, ssem, rsem, dev):
    return pltpu.make_async_remote_copy(
        src_ref=src, dst_ref=dst, send_sem=ssem, recv_sem=rsem, device_id=dev,
        device_id_type=pl.DeviceIdType.MESH,
    )


def kernel(
    d_ref, routes_ref, comb_ref, live_ref, hid_ref, out_ref,
    Z, R, S, HB, PB, SC, M, CN, RT, ACC, YS, YV,
    lsem, psem, prx, hsem, hps, hrx, mps, mrx, zs, zx, ms, mx,
    xs, rx, ys, yx, cs, cx,
):
    g = lax.axis_index("grp")
    e = lax.axis_index("ep")
    y, c = g // 2, g % 2
    x, z = e // 8, e % 8
    h = z // 4
    oc = 1 - c

    mate = (y * 2 + oc, e)
    zp = (g, x * 8 + (z + 1) % 8)
    zm = (g, x * 8 + (z + 7) % 8)
    xp = (g, ((x + 1) % 4) * 8 + z)
    xm = (g, ((x + 3) % 4) * 8 + z)
    xo = (g, ((x + 2) % 4) * 8 + z)
    yp = (((y + 1) % 4) * 2 + c, e)
    ym = (((y + 3) % 4) * 2 + c, e)
    bx1 = (g, (x + 1 - 2 * (x % 2)) * 8 + z)
    bx2 = (g, (3 - x) * 8 + z)
    by1 = ((y + 1 - 2 * (y % 2)) * 2 + c, e)
    by2 = ((3 - y) * 2 + c, e)

    barrier = pltpu.get_barrier_semaphore()
    for dev in (mate, zp, zm, xp, xm, xo, yp, ym):
        pl.semaphore_signal(barrier, inc=1, device_id=dev, device_id_type=pl.DeviceIdType.MESH)

    def column(i, half, core):
        dest = ((y + 2) % 4, None, None, y)[i]
        if dest is None:
            dest = (y + 1) % 4 if half == 0 else (y + 3) % 4
            off = 0 if i == 1 else HALF
        else:
            off = half * HALF
        return pl.ds(pl.multiple_of(WIDE * (2 * dest + core) + off, HALF), HALF)

    mine = pl.ds(pl.multiple_of(c * TOK, TOK), TOK)
    his = pl.ds(pl.multiple_of(oc * TOK, TOK), TOK)

    def source(b):
        hop = (b + 1) // 2
        return (z + 8 - hop) % 8 if b % 2 else (z + hop) % 8

    for i in range(CHUNKS):
        for half in range(2):
            pltpu.make_async_copy(
                d_ref.at[:, column(i, half, c)],
                Z.at[i, z, mine, pl.ds(half * HALF, HALF)],
                lsem.at[i],
            ).start()
    for b in range(8):
        pltpu.make_async_copy(hid_ref.at[:, source(b)], HB.at[b, c], hsem).start()

    er = lax.broadcasted_iota(jnp.int32, (EXPERTS, TOK), 0)
    tok = lax.broadcasted_iota(jnp.int32, (EXPERTS, TOK), 1)
    first = routes_ref[0:1, :] == er
    second = routes_ref[1:2, :] == er
    chosen = jnp.where(first, 1.0, 0.0) + jnp.where(second, 1.0, 0.0)
    before = (
        lax.broadcasted_iota(jnp.int32, (TOK, TOK), 0)
        < lax.broadcasted_iota(jnp.int32, (TOK, TOK), 1)
    )
    position = jnp.dot(
        chosen.astype(BF), jnp.where(before, 1.0, 0.0).astype(BF), preferred_element_type=F32
    )
    alive = jnp.where(tok < live_ref[...], chosen, 0.0)
    M[z, c, 0:8, :] = jnp.where(alive > 0.0, position, -1.0)
    M[z, c, 8:16, :] = jnp.where(first, comb_ref[0:1, :], 0.0) + jnp.where(
        second, comb_ref[1:2, :], 0.0
    )

    pl.semaphore_wait(barrier, 8)

    rcopy(M.at[z, c], M.at[z, c], mps, mrx, mate).start()
    for i in range(CHUNKS):
        for half in range(2):
            rcopy(
                d_ref.at[:, column(i, half, oc)],
                Z.at[i, z, mine, pl.ds(half * HALF, HALF)],
                psem, prx.at[i], mate,
            ).start()
    for b in range(8):
        rcopy(hid_ref.at[:, source(b)], HB.at[b, c], hps, hrx, mate).start()

    slot_iota = lax.broadcasted_iota(jnp.int32, (CAP, TOK), 0).astype(F32)

    def build_p(b, zz):
        for cc in range(2):
            for k in range(4):
                ex = 2 * ((x + k) % 4) + h
                hit = slot_iota == M[zz, cc, pl.ds(ex, 1), :]
                weight = jnp.where(hit, M[zz, cc, pl.ds(8 + ex, 1), :], 0.0)
                PB[b, cc, CAP * k:CAP * (k + 1), :] = jnp.where(hit, 1.0, 0.0).astype(BF)
                SC[b, cc, CAP * k:CAP * (k + 1), :] = jnp.broadcast_to(
                    jnp.sum(weight, axis=1, keepdims=True), (CAP, TOK)
                )

    def wave(b):
        return 0 if b < 5 else 1 if b < 7 else 2

    def process(*units):
        for i, b, zz in units:
            if i == 0:
                build_p(b, zz)

        for i, b, zz in units:
            for cc in range(2):
                picked = jnp.dot(
                    PB[b, cc], Z[i, zz, cc * TOK:(cc + 1) * TOK, :], preferred_element_type=F32
                )
                scale = SC[b, cc]
                slots = (picked * jnp.concatenate([scale, scale], axis=1)).astype(BF)
                R[i, b, cc, x] = slots[0:CAP]
                for k in range(1, 4):
                    S[i, b, k - 1, cc] = slots[CAP * k:CAP * (k + 1)]
        for i, b, zz in units:
            for k, dev in ((1, xo), (0, xp), (2, xm)):
                rcopy(S.at[i, b, k], R.at[i, b, :, x], xs, rx.at[i, k, wave(b)], dev).start()

    def zsend(i, zz, side, hop, whole):
        dev = (zp, zm)[side]
        ref = Z.at[i, zz] if whole else Z.at[i, zz, pl.ds(side * TOK, TOK)]
        rcopy(ref, ref, zs, zx.at[i, side, hop - 1], dev).start()

    def zwait(i, zz, side, hop, whole):
        dev = (zp, zm)[side]
        ref = Z.at[i, zz] if whole else Z.at[i, zz, pl.ds(side * TOK, TOK)]
        rcopy(ref, ref, zs, zx.at[i, side, hop - 1], dev).wait_recv()

    def msend(zz, side, hop, whole):
        dev = (zp, zm)[side]
        ref = M.at[zz] if whole else M.at[zz, side]
        rcopy(ref, ref, ms, mx.at[side, hop - 1], dev).start()

    def mwait(zz, side, hop, whole):
        dev = (zp, zm)[side]
        ref = M.at[zz] if whole else M.at[zz, side]
        rcopy(ref, ref, ms, mx.at[side, hop - 1], dev).wait_recv()

    def away(hop, side):
        return (z + 8 - hop) % 8 if side == 0 else (z + hop) % 8

    def ready(i):
        pltpu.make_async_copy(Z.at[i, z, mine], Z.at[i, z, mine], lsem.at[i]).wait()
        rcopy(Z.at[i, z, his], Z.at[i, z, his], psem, prx.at[i], mate).wait_recv()

    def z0(i):
        for side in range(2):
            zsend(i, z, side, 1, True)

    def own(i):
        ready(i)
        process((i, 0, z))

    def zhop(i, hop):
        for side in range(2):
            block = away(hop, side)

            if i == 0:
                mwait(block, side, hop, True)
                msend(block, side, hop + 1, hop < 3)

            zwait(i, block, side, hop, True)
            zsend(i, block, side, hop + 1, hop < 3)

    def z4(i):
        block = away(4, 1)

        if i == 0:
            for side in range(2):
                mwait(block, side, 4, False)

        for side in range(2):
            zwait(i, block, side, 4, False)

    def both_sides(i, hop):
        process((i, 2 * hop - 1, away(hop, 0)), (i, 2 * hop, away(hop, 1)))

    def arrive(ch, w):
        lo, hi = ((0, 5), (5, 7), (7, 8))[w]
        for k in range(3):
            ref = R.at[ch, lo:hi, :, 0]
            rcopy(ref, ref, xs, rx.at[ch, k, w], (xp, xo, xm)[k]).wait_recv()

    def turn(ch, lo, hi):
        @pl.loop(lo, hi)
        def _(b):
            cols = pl.ds(pl.multiple_of(b * KB, KB), KB)
            RT[:, cols] = R[ch, b].reshape(KB, WIDE).T

    def partial(lo, hi, cols):
        right = HB[lo:hi, :, :, :, cols].reshape((hi - lo) * KB, 256)
        return jnp.dot(RT[:, lo * KB:hi * KB], right, preferred_element_type=F32)

    def column_tiles(body):
        @pl.loop(0, 7)
        def _(n):
            body(pl.ds(pl.multiple_of(n * 256, 256), 256))

    def multiply_first(ch):
        arrive(ch, 0)
        turn(ch, 0, 5)

        @column_tiles
        def _(cols):
            ACC[:, cols] = partial(0, 5, cols)

    def multiply_rest(ch):
        arrive(ch, 1)
        arrive(ch, 2)
        turn(ch, 5, 8)

        @column_tiles
        def _(cols):
            ACC[:, cols] += partial(5, 8, cols)

    def ywait(ch, half):
        ref = YV.at[ch, half]
        rcopy(ref, ref, ys, yx.at[ch, half], (yp, ym)[half]).wait_recv()

    def reduce_send(ch):
        for half in range(2):
            @pl.when(ch == half + 1)
            def _():
                ywait(0, half)

                @pl.loop(0, 7)
                def _(n):
                    cols = pl.ds(pl.multiple_of(n * 256, 256), 256)
                    ACC[half * HALF:(half + 1) * HALF, cols] += YV[0, half, :, cols].astype(F32)

            @pl.loop(0, 7)
            def _(n):
                cols = pl.ds(pl.multiple_of(n * 256, 256), 256)
                YS[ch, half, :, cols] = ACC[half * HALF:(half + 1) * HALF, cols].astype(BF)

            rcopy(YS.at[ch, half], YV.at[ch, half], ys, yx.at[ch, half], (yp, ym)[half]).start()

    def count_send(step):
        dev = (bx1, bx2, by1, by2)[step]
        rcopy(CN.at[0, step], CN.at[1, step], cs, cx.at[step], dev).start()

    def count_wait(step):
        dev = (bx1, bx2, by1, by2)[step]
        rcopy(CN.at[1, step], CN.at[1, step], cs, cx.at[step], dev).wait_recv()
        return CN[0, step] + CN[1, step]

    rcopy(M.at[z, oc], M.at[z, oc], mps, mrx, mate).wait_recv()
    for side in range(2):
        msend(z, side, 1, True)

    ready(0)


    def blocks(i, hop):
        if hop == 0:
            process((i, 0, z))
        elif hop == 4:
            process((i, 7, away(4, 1)))
        else:
            both_sides(i, hop)

    def along_z(i, hop):
        if hop == 0:
            z0(i)
        elif hop == 4:
            z4(i)
        else:
            zhop(i, hop)

    def count_step(k):
        if k == 0:
            total = jnp.zeros((EXPERTS, TOK), F32)
            for zz in range(8):
                for cc in range(2):
                    total += jnp.where(M[zz, cc, 0:8, :] >= 0.0, 1.0, 0.0)
            CN[0, 0] = total
        else:
            CN[0, k] = count_wait(k - 1)
        count_send(k)

    def hidden_here():
        pltpu.make_async_copy(HB.at[:, c], HB.at[:, c], hsem).wait()
        rcopy(HB.at[:, oc], HB.at[:, oc], hps, hrx, mate).wait_recv()

    def multiply_last(ch):
        multiply_rest(ch)
        reduce_send(ch)

    acts = dict(
        r=ready, z=along_z, p=blocks, c=count_step, h=hidden_here, f=multiply_first,
        l=multiply_last,
    )
    for step in PLAN:
        acts[step[0]](*map(int, step[1:]))

    multiply_first(3)
    total = count_wait(3)
    picked = jnp.where(er == 2 * x + h, total, 0.0)
    count = jnp.sum(jnp.sum(picked, axis=1, keepdims=True), axis=0, keepdims=True)
    factor = lax.rsqrt(1.0 + count)
    arrive(3, 1)
    turn(3, 5, 7)
    for ch in (1, 2):
        for half in range(2):
            ywait(ch, half)

    @column_tiles
    def _(cols):
        ACC[:, cols] += partial(5, 7, cols)
        for part in range(2):
            rows = slice(part * HALF, (part + 1) * HALF)
            ACC[rows, cols] += YV[part + 1, 0, :, cols].astype(F32) + YV[
                part + 1, 1, :, cols
            ].astype(F32)

    arrive(3, 2)
    turn(3, 7, 8)

    @column_tiles
    def _(cols):
        out_ref[:, cols] = (ACC[:, cols] + partial(7, 8, cols)) * factor

    rcopy(M.at[z, c], M.at[z, c], mps, mrx, mate).wait_send()
    sent = Z.at[:, 0, pl.ds(0, TOK)]
    rcopy(sent, sent, psem, prx.at[0], mate).wait_send()
    rcopy(HB.at[:, c], HB.at[:, c], hps, hrx, mate).wait_send()
    sent = M.at[pl.ds(0, 7)]
    rcopy(sent, sent, ms, mx.at[0, 0], zp).wait_send()
    sent = Z.at[:, pl.ds(0, 7)]
    rcopy(sent, sent, zs, zx.at[0, 0, 0], zp).wait_send()
    rcopy(S, S, xs, rx.at[0, 0, 0], xp).wait_send()
    rcopy(YS, YS, ys, yx.at[0, 0], yp).wait_send()
    rcopy(CN.at[0], CN.at[0], cs, cx.at[0], bx1).wait_send()


def on_device(d_out, routes, combine, live_tokens, hidden):
    dma = pltpu.SemaphoreType.DMA
    any_spec = pl.BlockSpec(memory_space=pl.ANY)
    vmem = pl.BlockSpec(memory_space=pltpu.VMEM)
    return pl.pallas_call(
        kernel,
        out_shape=jax.ShapeDtypeStruct((WIDE, 1792), F32),
        in_specs=[any_spec, vmem, vmem, vmem, any_spec],
        out_specs=vmem,
        scratch_shapes=[
            pltpu.VMEM((CHUNKS, 8, 2 * TOK, WIDE), BF),
            pltpu.VMEM((CHUNKS, 8, 2, 4, CAP, WIDE), BF),
            pltpu.VMEM((CHUNKS, 8, 3, 2, CAP, WIDE), BF),
            pltpu.VMEM((8, 2, 4, CAP, 1792), BF),
            pltpu.VMEM((8, 2, 4 * CAP, TOK), BF),
            pltpu.VMEM((8, 2, 4 * CAP, TOK), F32),
            pltpu.VMEM((8, 2, 16, TOK), F32),
            pltpu.VMEM((2, 4, EXPERTS, TOK), F32),
            pltpu.VMEM((WIDE, 2 * 1536), BF),
            pltpu.VMEM((WIDE, 1792), F32),
            pltpu.VMEM((3, 2, HALF, 1792), BF),
            pltpu.VMEM((3, 2, HALF, 1792), BF),
            dma((CHUNKS,)), dma, dma((CHUNKS,)), dma, dma, dma, dma, dma,
            dma, dma((CHUNKS, 2, 4)), dma, dma((2, 4)),
            dma, dma((CHUNKS, 3, 3)),
            dma, dma((3, 2)), dma, dma((4,)),
        ],
        compiler_params=pltpu.CompilerParams(
            collective_id=0, has_side_effects=True, vmem_limit_bytes=54000000
        ),
    )(d_out, routes.T, combine.T, live_tokens.reshape(1, 1), hidden.reshape(4, 8, CAP, 1792))


def solution(mesh):
    both = P(("grp", "ep"), None)
    return jax.shard_map(
        on_device, mesh=mesh,
        in_specs=(both, both, both, P(("grp", "ep")), P("grp", "ep")),
        out_specs=P("grp", "ep"), check_vma=False,
    )
```

```python
import functools

import jax
import jax.numpy as jnp
from jax import lax
from jax.experimental import pallas as pl
from jax.experimental.pallas import tpu as pltpu
from jax.sharding import PartitionSpec as P

EXPERTS = 8
CAP = 48
TOK = 128
CHUNKS = 4
WIDE = 256
HALF = 128
PLAN = (
    "z00", "p00", "r1", "p10", "r3",
    "z01", "p01", "r2", "p20",
    "z02", "z10", "p02",
    "z03", "z11", "p03", "p11",
    "z04", "z12", "z20", "p04", "p12", "c0", "h", "f0",
    "z13", "z21", "p13", "p21", "l0",
    "z14", "z22", "z30", "p14", "p22", "c1", "f1",
    "z23", "z31", "p23", "p30", "c2", "l1",
    "z24", "z32", "p24", "p31", "p32", "c3", "f2",
    "z33", "p33", "l2",
    "z34", "p34",
)
KB = 8 * CAP
BF = jnp.bfloat16
F32 = jnp.float32


def rcopy(src, dst, ssem, rsem, dev):
    return pltpu.make_async_remote_copy(
        src_ref=src, dst_ref=dst, send_sem=ssem, recv_sem=rsem, device_id=dev,
        device_id_type=pl.DeviceIdType.MESH,
    )


def kernel(
    d_ref, routes_ref, comb_ref, live_ref, hid_ref, out_ref,
    Z, R, S, HB, PB, SC, M, CN, RT, ACC, YS, YV,
    lsem, psem, prx, hsem, hps, hrx, mps, mrx, zs, zx, ms, mx,
    xs, rx, ys, yx, cs, cx,
):
    g = lax.axis_index("grp")
    e = lax.axis_index("ep")
    y, c = g // 2, g % 2
    x, z = e // 8, e % 8
    h = z // 4
    oc = 1 - c

    mate = (y * 2 + oc, e)
    zp = (g, x * 8 + (z + 1) % 8)
    zm = (g, x * 8 + (z + 7) % 8)
    xp = (g, ((x + 1) % 4) * 8 + z)
    xm = (g, ((x + 3) % 4) * 8 + z)
    xo = (g, ((x + 2) % 4) * 8 + z)
    yp = (((y + 1) % 4) * 2 + c, e)
    ym = (((y + 3) % 4) * 2 + c, e)
    bx1 = (g, (x + 1 - 2 * (x % 2)) * 8 + z)
    bx2 = (g, (3 - x) * 8 + z)
    by1 = ((y + 1 - 2 * (y % 2)) * 2 + c, e)
    by2 = ((3 - y) * 2 + c, e)

    barrier = pltpu.get_barrier_semaphore()
    for dev in (mate, zp, zm, xp, xm, xo, yp, ym):
        pl.semaphore_signal(barrier, inc=1, device_id=dev, device_id_type=pl.DeviceIdType.MESH)

    def column(i, half, core):
        dest = ((y + 2) % 4, None, None, y)[i]
        if dest is None:
            dest = (y + 1) % 4 if half == 0 else (y + 3) % 4
            off = 0 if i == 1 else HALF
        else:
            off = half * HALF
        return pl.ds(pl.multiple_of(WIDE * (2 * dest + core) + off, HALF), HALF)

    mine = pl.ds(pl.multiple_of(c * TOK, TOK), TOK)
    his = pl.ds(pl.multiple_of(oc * TOK, TOK), TOK)

    def source(b):
        hop = (b + 1) // 2
        return (z + 8 - hop) % 8 if b % 2 else (z + hop) % 8

    for i in range(CHUNKS):
        for half in range(2):
            pltpu.make_async_copy(
                d_ref.at[:, column(i, half, c)],
                Z.at[i, z, mine, pl.ds(half * HALF, HALF)],
                lsem.at[i],
            ).start()
    for b in range(8):
        pltpu.make_async_copy(hid_ref.at[:, source(b)], HB.at[b, c], hsem).start()

    er = lax.broadcasted_iota(jnp.int32, (EXPERTS, TOK), 0)
    tok = lax.broadcasted_iota(jnp.int32, (EXPERTS, TOK), 1)
    first = routes_ref[0:1, :] == er
    second = routes_ref[1:2, :] == er
    chosen = jnp.where(first, 1.0, 0.0) + jnp.where(second, 1.0, 0.0)
    before = (
        lax.broadcasted_iota(jnp.int32, (TOK, TOK), 0)
        < lax.broadcasted_iota(jnp.int32, (TOK, TOK), 1)
    )
    position = jnp.dot(
        chosen.astype(BF), jnp.where(before, 1.0, 0.0).astype(BF), preferred_element_type=F32
    )
    alive = jnp.where(tok < live_ref[...], chosen, 0.0)
    M[z, c, 0:8, :] = jnp.where(alive > 0.0, position, -1.0)
    M[z, c, 8:16, :] = jnp.where(first, comb_ref[0:1, :], 0.0) + jnp.where(
        second, comb_ref[1:2, :], 0.0
    )

    pl.semaphore_wait(barrier, 8)

    rcopy(M.at[z, c], M.at[z, c], mps, mrx, mate).start()
    for i in range(CHUNKS):
        for half in range(2):
            rcopy(
                d_ref.at[:, column(i, half, oc)],
                Z.at[i, z, mine, pl.ds(half * HALF, HALF)],
                psem, prx.at[i], mate,
            ).start()
    for b in range(8):
        rcopy(hid_ref.at[:, source(b)], HB.at[b, c], hps, hrx, mate).start()

    slot_iota = lax.broadcasted_iota(jnp.int32, (CAP, TOK), 0).astype(F32)

    def build_p(b, zz):
        for cc in range(2):
            for k in range(4):
                ex = 2 * ((x + k) % 4) + h
                hit = slot_iota == M[zz, cc, pl.ds(ex, 1), :]
                weight = jnp.where(hit, M[zz, cc, pl.ds(8 + ex, 1), :], 0.0)
                PB[b, cc, CAP * k:CAP * (k + 1), :] = jnp.where(hit, 1.0, 0.0).astype(BF)
                SC[b, cc, CAP * k:CAP * (k + 1), :] = jnp.broadcast_to(
                    jnp.sum(weight, axis=1, keepdims=True), (CAP, TOK)
                )

    def wave(b):
        return 0 if b < 5 else 1 if b < 7 else 2

    def process(*units):
        for i, b, zz in units:
            if i == 0:
                build_p(b, zz)

        for i, b, zz in units:
            for cc in range(2):
                picked = jnp.dot(
                    PB[b, cc], Z[i, zz, cc * TOK:(cc + 1) * TOK, :], preferred_element_type=F32
                )
                scale = SC[b, cc]
                slots = (picked * jnp.concatenate([scale, scale], axis=1)).astype(BF)
                R[i, b, cc, x] = slots[0:CAP]
                for k in range(1, 4):
                    S[i, b, k - 1, cc] = slots[CAP * k:CAP * (k + 1)]
        for i, b, zz in units:
            for k, dev in ((1, xo), (0, xp), (2, xm)):
                rcopy(S.at[i, b, k], R.at[i, b, :, x], xs, rx.at[i, k, wave(b)], dev).start()

    def zsend(i, zz, side, hop, whole):
        dev = (zp, zm)[side]
        ref = Z.at[i, zz] if whole else Z.at[i, zz, pl.ds(side * TOK, TOK)]
        rcopy(ref, ref, zs, zx.at[i, side, hop - 1], dev).start()

    def zwait(i, zz, side, hop, whole):
        dev = (zp, zm)[side]
        ref = Z.at[i, zz] if whole else Z.at[i, zz, pl.ds(side * TOK, TOK)]
        rcopy(ref, ref, zs, zx.at[i, side, hop - 1], dev).wait_recv()

    def msend(zz, side, hop, whole):
        dev = (zp, zm)[side]
        ref = M.at[zz] if whole else M.at[zz, side]
        rcopy(ref, ref, ms, mx.at[side, hop - 1], dev).start()

    def mwait(zz, side, hop, whole):
        dev = (zp, zm)[side]
        ref = M.at[zz] if whole else M.at[zz, side]
        rcopy(ref, ref, ms, mx.at[side, hop - 1], dev).wait_recv()

    def away(hop, side):
        return (z + 8 - hop) % 8 if side == 0 else (z + hop) % 8

    def ready(i):
        pltpu.make_async_copy(Z.at[i, z, mine], Z.at[i, z, mine], lsem.at[i]).wait()
        rcopy(Z.at[i, z, his], Z.at[i, z, his], psem, prx.at[i], mate).wait_recv()

    def z0(i):
        for side in range(2):
            zsend(i, z, side, 1, True)

    def own(i):
        ready(i)
        process((i, 0, z))

    def zhop(i, hop):
        for side in range(2):
            block = away(hop, side)

            if i == 0:
                mwait(block, side, hop, True)
                msend(block, side, hop + 1, hop < 3)

            zwait(i, block, side, hop, True)
            zsend(i, block, side, hop + 1, hop < 3)

    def z4(i):
        block = away(4, 1)

        if i == 0:
            for side in range(2):
                mwait(block, side, 4, False)

        for side in range(2):
            zwait(i, block, side, 4, False)

    def both_sides(i, hop):
        process((i, 2 * hop - 1, away(hop, 0)), (i, 2 * hop, away(hop, 1)))

    def arrive(ch, w):
        lo, hi = ((0, 5), (5, 7), (7, 8))[w]
        for k in range(3):
            ref = R.at[ch, lo:hi, :, 0]
            rcopy(ref, ref, xs, rx.at[ch, k, w], (xp, xo, xm)[k]).wait_recv()

    def turn(ch, lo, hi):
        @pl.loop(lo, hi)
        def _(b):
            cols = pl.ds(pl.multiple_of(b * KB, KB), KB)
            RT[:, cols] = R[ch, b].reshape(KB, WIDE).T

    def partial(lo, hi, cols):
        right = HB[lo:hi, :, :, :, cols].reshape((hi - lo) * KB, 256)
        return jnp.dot(RT[:, lo * KB:hi * KB], right, preferred_element_type=F32)

    def column_tiles(body):
        @pl.loop(0, 7)
        def _(n):
            body(pl.ds(pl.multiple_of(n * 256, 256), 256))

    def multiply_first(ch):
        arrive(ch, 0)
        turn(ch, 0, 5)

        @column_tiles
        def _(cols):
            ACC[:, cols] = partial(0, 5, cols)

    def multiply_rest(ch):
        arrive(ch, 1)
        arrive(ch, 2)
        turn(ch, 5, 8)

        @column_tiles
        def _(cols):
            ACC[:, cols] += partial(5, 8, cols)

    def ywait(ch, half):
        ref = YV.at[ch, half]
        rcopy(ref, ref, ys, yx.at[ch, half], (yp, ym)[half]).wait_recv()

    def reduce_send(ch):
        for half in range(2):
            @pl.when(ch == half + 1)
            def _():
                ywait(0, half)

                @pl.loop(0, 7)
                def _(n):
                    cols = pl.ds(pl.multiple_of(n * 256, 256), 256)
                    ACC[half * HALF:(half + 1) * HALF, cols] += YV[0, half, :, cols].astype(F32)

            @pl.loop(0, 7)
            def _(n):
                cols = pl.ds(pl.multiple_of(n * 256, 256), 256)
                YS[ch, half, :, cols] = ACC[half * HALF:(half + 1) * HALF, cols].astype(BF)

            rcopy(YS.at[ch, half], YV.at[ch, half], ys, yx.at[ch, half], (yp, ym)[half]).start()

    def count_send(step):
        dev = (bx1, bx2, by1, by2)[step]
        rcopy(CN.at[0, step], CN.at[1, step], cs, cx.at[step], dev).start()

    def count_wait(step):
        dev = (bx1, bx2, by1, by2)[step]
        rcopy(CN.at[1, step], CN.at[1, step], cs, cx.at[step], dev).wait_recv()
        return CN[0, step] + CN[1, step]

    rcopy(M.at[z, oc], M.at[z, oc], mps, mrx, mate).wait_recv()
    for side in range(2):
        msend(z, side, 1, True)

    ready(0)


    def blocks(i, hop):
        if hop == 0:
            process((i, 0, z))
        elif hop == 4:
            process((i, 7, away(4, 1)))
        else:
            both_sides(i, hop)

    def along_z(i, hop):
        if hop == 0:
            z0(i)
        elif hop == 4:
            z4(i)
        else:
            zhop(i, hop)

    def count_step(k):
        if k == 0:
            total = jnp.zeros((EXPERTS, TOK), F32)
            for zz in range(8):
                for cc in range(2):
                    total += jnp.where(M[zz, cc, 0:8, :] >= 0.0, 1.0, 0.0)
            CN[0, 0] = total
        else:
            CN[0, k] = count_wait(k - 1)
        count_send(k)

    def hidden_here():
        pltpu.make_async_copy(HB.at[:, c], HB.at[:, c], hsem).wait()
        rcopy(HB.at[:, oc], HB.at[:, oc], hps, hrx, mate).wait_recv()

    def multiply_last(ch):
        multiply_rest(ch)
        reduce_send(ch)

    acts = dict(
        r=ready, z=along_z, p=blocks, c=count_step, h=hidden_here, f=multiply_first,
        l=multiply_last,
    )
    for step in PLAN:
        acts[step[0]](*map(int, step[1:]))

    multiply_first(3)
    total = count_wait(3)
    picked = jnp.where(er == 2 * x + h, total, 0.0)
    count = jnp.sum(jnp.sum(picked, axis=1, keepdims=True), axis=0, keepdims=True)
    factor = lax.rsqrt(1.0 + count)
    arrive(3, 1)
    turn(3, 5, 7)
    for half in range(2):
        ywait(1, half)

    def groups(part, cols):
        return YV[part + 1, 0, :, cols].astype(F32) + YV[part + 1, 1, :, cols].astype(F32)

    @column_tiles
    def _(cols):
        ACC[:, cols] += partial(5, 7, cols)
        ACC[:HALF, cols] += groups(0, cols)

    arrive(3, 2)
    turn(3, 7, 8)
    for half in range(2):
        ywait(2, half)

    @column_tiles
    def _(cols):
        last = ACC[:, cols] + partial(7, 8, cols)
        out_ref[:HALF, cols] = last[:HALF] * factor
        out_ref[HALF:, cols] = (last[HALF:] + groups(1, cols)) * factor

    rcopy(M.at[z, c], M.at[z, c], mps, mrx, mate).wait_send()
    sent = Z.at[:, 0, pl.ds(0, TOK)]
    rcopy(sent, sent, psem, prx.at[0], mate).wait_send()
    rcopy(HB.at[:, c], HB.at[:, c], hps, hrx, mate).wait_send()
    sent = M.at[pl.ds(0, 7)]
    rcopy(sent, sent, ms, mx.at[0, 0], zp).wait_send()
    sent = Z.at[:, pl.ds(0, 7)]
    rcopy(sent, sent, zs, zx.at[0, 0, 0], zp).wait_send()
    rcopy(S, S, xs, rx.at[0, 0, 0], xp).wait_send()
    rcopy(YS, YS, ys, yx.at[0, 0], yp).wait_send()
    rcopy(CN.at[0], CN.at[0], cs, cx.at[0], bx1).wait_send()


def on_device(d_out, routes, combine, live_tokens, hidden):
    dma = pltpu.SemaphoreType.DMA
    any_spec = pl.BlockSpec(memory_space=pl.ANY)
    vmem = pl.BlockSpec(memory_space=pltpu.VMEM)
    return pl.pallas_call(
        kernel,
        out_shape=jax.ShapeDtypeStruct((WIDE, 1792), F32),
        in_specs=[any_spec, vmem, vmem, vmem, any_spec],
        out_specs=vmem,
        scratch_shapes=[
            pltpu.VMEM((CHUNKS, 8, 2 * TOK, WIDE), BF),
            pltpu.VMEM((CHUNKS, 8, 2, 4, CAP, WIDE), BF),
            pltpu.VMEM((CHUNKS, 8, 3, 2, CAP, WIDE), BF),
            pltpu.VMEM((8, 2, 4, CAP, 1792), BF),
            pltpu.VMEM((8, 2, 4 * CAP, TOK), BF),
            pltpu.VMEM((8, 2, 4 * CAP, TOK), F32),
            pltpu.VMEM((8, 2, 16, TOK), F32),
            pltpu.VMEM((2, 4, EXPERTS, TOK), F32),
            pltpu.VMEM((WIDE, 2 * 1536), BF),
            pltpu.VMEM((WIDE, 1792), F32),
            pltpu.VMEM((3, 2, HALF, 1792), BF),
            pltpu.VMEM((3, 2, HALF, 1792), BF),
            dma((CHUNKS,)), dma, dma((CHUNKS,)), dma, dma, dma, dma, dma,
            dma, dma((CHUNKS, 2, 4)), dma, dma((2, 4)),
            dma, dma((CHUNKS, 3, 3)),
            dma, dma((3, 2)), dma, dma((4,)),
        ],
        compiler_params=pltpu.CompilerParams(
            collective_id=0, has_side_effects=True, vmem_limit_bytes=54000000
        ),
    )(d_out, routes.T, combine.T, live_tokens.reshape(1, 1), hidden.reshape(4, 8, CAP, 1792))


def solution(mesh):
    both = P(("grp", "ep"), None)
    return jax.shard_map(
        on_device, mesh=mesh,
        in_specs=(both, both, both, P(("grp", "ep")), P("grp", "ep")),
        out_specs=P("grp", "ep"), check_vma=False,
    )
```

```python
import functools

import jax
import jax.numpy as jnp
from jax import lax
from jax.experimental import pallas as pl
from jax.experimental.pallas import tpu as pltpu
from jax.sharding import PartitionSpec as P

EXPERTS = 8
CAP = 48
TOK = 128
CHUNKS = 4
WIDE = 256
HALF = 128
PLAN = (
    "z00", "p00", "r1", "p10", "r2", "p20", "r3",
    "z01", "p01",
    "z02", "z10", "p02",
    "z03", "z11", "p03", "p11",
    "z04", "z12", "z20", "p04", "p12", "c0", "h", "f0",
    "z13", "z21", "p13", "p21", "l0",
    "z14", "z22", "z30", "p14", "p22", "c1", "f1",
    "z23", "z31", "p23", "p30", "c2", "l1",
    "z24", "z32", "p24", "p31", "p32", "c3", "f2",
    "z33", "p33", "l2",
    "z34", "p34",
)
KB = 8 * CAP
BF = jnp.bfloat16
F32 = jnp.float32


def rcopy(src, dst, ssem, rsem, dev):
    return pltpu.make_async_remote_copy(
        src_ref=src, dst_ref=dst, send_sem=ssem, recv_sem=rsem, device_id=dev,
        device_id_type=pl.DeviceIdType.MESH,
    )


def kernel(
    d_ref, routes_ref, comb_ref, live_ref, hid_ref, out_ref,
    Z, R, S, HB, PB, SC, M, CN, RT, ACC, YS, YV,
    lsem, psem, prx, hsem, hps, hrx, mps, mrx, zs, zx, ms, mx,
    xs, rx, ys, yx, cs, cx,
):
    g = lax.axis_index("grp")
    e = lax.axis_index("ep")
    y, c = g // 2, g % 2
    x, z = e // 8, e % 8
    h = z // 4
    oc = 1 - c

    mate = (y * 2 + oc, e)
    zp = (g, x * 8 + (z + 1) % 8)
    zm = (g, x * 8 + (z + 7) % 8)
    xp = (g, ((x + 1) % 4) * 8 + z)
    xm = (g, ((x + 3) % 4) * 8 + z)
    xo = (g, ((x + 2) % 4) * 8 + z)
    yp = (((y + 1) % 4) * 2 + c, e)
    ym = (((y + 3) % 4) * 2 + c, e)
    bx1 = (g, (x + 1 - 2 * (x % 2)) * 8 + z)
    bx2 = (g, (3 - x) * 8 + z)
    by1 = ((y + 1 - 2 * (y % 2)) * 2 + c, e)
    by2 = ((3 - y) * 2 + c, e)

    barrier = pltpu.get_barrier_semaphore()
    for dev in (mate, zp, zm, xp, xm, xo, yp, ym):
        pl.semaphore_signal(barrier, inc=1, device_id=dev, device_id_type=pl.DeviceIdType.MESH)

    def column(i, half, core):
        dest = ((y + 2) % 4, None, None, y)[i]
        if dest is None:
            dest = (y + 1) % 4 if half == 0 else (y + 3) % 4
            off = 0 if i == 1 else HALF
        else:
            off = half * HALF
        return pl.ds(pl.multiple_of(WIDE * (2 * dest + core) + off, HALF), HALF)

    mine = pl.ds(pl.multiple_of(c * TOK, TOK), TOK)
    his = pl.ds(pl.multiple_of(oc * TOK, TOK), TOK)

    def source(b):
        hop = (b + 1) // 2
        return (z + 8 - hop) % 8 if b % 2 else (z + hop) % 8

    for i in range(CHUNKS):
        for half in range(2):
            pltpu.make_async_copy(
                d_ref.at[:, column(i, half, c)],
                Z.at[i, z, mine, pl.ds(half * HALF, HALF)],
                lsem.at[i],
            ).start()
    for b in range(8):
        pltpu.make_async_copy(hid_ref.at[:, source(b)], HB.at[b, c], hsem).start()

    er = lax.broadcasted_iota(jnp.int32, (EXPERTS, TOK), 0)
    tok = lax.broadcasted_iota(jnp.int32, (EXPERTS, TOK), 1)
    first = routes_ref[0:1, :] == er
    second = routes_ref[1:2, :] == er
    chosen = jnp.where(first, 1.0, 0.0) + jnp.where(second, 1.0, 0.0)
    before = (
        lax.broadcasted_iota(jnp.int32, (TOK, TOK), 0)
        < lax.broadcasted_iota(jnp.int32, (TOK, TOK), 1)
    )
    position = jnp.dot(
        chosen.astype(BF), jnp.where(before, 1.0, 0.0).astype(BF), preferred_element_type=F32
    )
    alive = jnp.where(tok < live_ref[...], chosen, 0.0)
    M[z, c, 0:8, :] = jnp.where(alive > 0.0, position, -1.0)
    M[z, c, 8:16, :] = jnp.where(first, comb_ref[0:1, :], 0.0) + jnp.where(
        second, comb_ref[1:2, :], 0.0
    )

    pl.semaphore_wait(barrier, 8)

    rcopy(M.at[z, c], M.at[z, c], mps, mrx, mate).start()
    for i in range(CHUNKS):
        for half in range(2):
            rcopy(
                d_ref.at[:, column(i, half, oc)],
                Z.at[i, z, mine, pl.ds(half * HALF, HALF)],
                psem, prx.at[i], mate,
            ).start()
    for b in range(8):
        rcopy(hid_ref.at[:, source(b)], HB.at[b, c], hps, hrx, mate).start()

    slot_iota = lax.broadcasted_iota(jnp.int32, (CAP, TOK), 0).astype(F32)

    def build_p(b, zz):
        for cc in range(2):
            for k in range(4):
                ex = 2 * ((x + k) % 4) + h
                hit = slot_iota == M[zz, cc, pl.ds(ex, 1), :]
                weight = jnp.where(hit, M[zz, cc, pl.ds(8 + ex, 1), :], 0.0)
                PB[b, cc, CAP * k:CAP * (k + 1), :] = jnp.where(hit, 1.0, 0.0).astype(BF)
                SC[b, cc, CAP * k:CAP * (k + 1), :] = jnp.broadcast_to(
                    jnp.sum(weight, axis=1, keepdims=True), (CAP, TOK)
                )

    def wave(b):
        return 0 if b < 5 else 1 if b < 7 else 2

    def process(*units):
        for i, b, zz in units:
            if i == 0:
                build_p(b, zz)

        for i, b, zz in units:
            for cc in range(2):
                picked = jnp.dot(
                    PB[b, cc], Z[i, zz, cc * TOK:(cc + 1) * TOK, :], preferred_element_type=F32
                )
                scale = SC[b, cc]
                slots = (picked * jnp.concatenate([scale, scale], axis=1)).astype(BF)
                R[i, b, cc, x] = slots[0:CAP]
                for k in range(1, 4):
                    S[i, b, k - 1, cc] = slots[CAP * k:CAP * (k + 1)]
        for i, b, zz in units:
            for k, dev in ((1, xo), (0, xp), (2, xm)):
                rcopy(S.at[i, b, k], R.at[i, b, :, x], xs, rx.at[i, k, wave(b)], dev).start()

    def zsend(i, zz, side, hop, whole):
        dev = (zp, zm)[side]
        ref = Z.at[i, zz] if whole else Z.at[i, zz, pl.ds(side * TOK, TOK)]
        rcopy(ref, ref, zs, zx.at[i, side, hop - 1], dev).start()

    def zwait(i, zz, side, hop, whole):
        dev = (zp, zm)[side]
        ref = Z.at[i, zz] if whole else Z.at[i, zz, pl.ds(side * TOK, TOK)]
        rcopy(ref, ref, zs, zx.at[i, side, hop - 1], dev).wait_recv()

    def msend(zz, side, hop, whole):
        dev = (zp, zm)[side]
        ref = M.at[zz] if whole else M.at[zz, side]
        rcopy(ref, ref, ms, mx.at[side, hop - 1], dev).start()

    def mwait(zz, side, hop, whole):
        dev = (zp, zm)[side]
        ref = M.at[zz] if whole else M.at[zz, side]
        rcopy(ref, ref, ms, mx.at[side, hop - 1], dev).wait_recv()

    def away(hop, side):
        return (z + 8 - hop) % 8 if side == 0 else (z + hop) % 8

    def ready(i):
        pltpu.make_async_copy(Z.at[i, z, mine], Z.at[i, z, mine], lsem.at[i]).wait()
        rcopy(Z.at[i, z, his], Z.at[i, z, his], psem, prx.at[i], mate).wait_recv()

    def z0(i):
        for side in range(2):
            zsend(i, z, side, 1, True)

    def own(i):
        ready(i)
        process((i, 0, z))

    def zhop(i, hop):
        for side in range(2):
            block = away(hop, side)

            if i == 0:
                mwait(block, side, hop, True)
                msend(block, side, hop + 1, hop < 3)

            zwait(i, block, side, hop, True)
            zsend(i, block, side, hop + 1, hop < 3)

    def z4(i):
        block = away(4, 1)

        if i == 0:
            for side in range(2):
                mwait(block, side, 4, False)

        for side in range(2):
            zwait(i, block, side, 4, False)

    def both_sides(i, hop):
        process((i, 2 * hop - 1, away(hop, 0)), (i, 2 * hop, away(hop, 1)))

    def arrive(ch, w):
        lo, hi = ((0, 5), (5, 7), (7, 8))[w]
        for k in range(3):
            ref = R.at[ch, lo:hi, :, 0]
            rcopy(ref, ref, xs, rx.at[ch, k, w], (xp, xo, xm)[k]).wait_recv()

    def turn(ch, lo, hi):
        @pl.loop(lo, hi)
        def _(b):
            cols = pl.ds(pl.multiple_of(b * KB, KB), KB)
            RT[:, cols] = R[ch, b].reshape(KB, WIDE).T

    def partial(lo, hi, cols):
        right = HB[lo:hi, :, :, :, cols].reshape((hi - lo) * KB, 256)
        return jnp.dot(RT[:, lo * KB:hi * KB], right, preferred_element_type=F32)

    def column_tiles(body):
        @pl.loop(0, 7)
        def _(n):
            body(pl.ds(pl.multiple_of(n * 256, 256), 256))

    def multiply_first(ch):
        arrive(ch, 0)
        turn(ch, 0, 5)

        @column_tiles
        def _(cols):
            ACC[:, cols] = partial(0, 5, cols)

    def multiply_rest(ch):
        arrive(ch, 1)
        arrive(ch, 2)
        turn(ch, 5, 8)

        @column_tiles
        def _(cols):
            ACC[:, cols] += partial(5, 8, cols)

    def ywait(ch, half):
        ref = YV.at[ch, half]
        rcopy(ref, ref, ys, yx.at[ch, half], (yp, ym)[half]).wait_recv()

    def reduce_send(ch):
        for half in range(2):
            @pl.when(ch == half + 1)
            def _():
                ywait(0, half)

                @pl.loop(0, 7)
                def _(n):
                    cols = pl.ds(pl.multiple_of(n * 256, 256), 256)
                    ACC[half * HALF:(half + 1) * HALF, cols] += YV[0, half, :, cols].astype(F32)

            @pl.loop(0, 7)
            def _(n):
                cols = pl.ds(pl.multiple_of(n * 256, 256), 256)
                YS[ch, half, :, cols] = ACC[half * HALF:(half + 1) * HALF, cols].astype(BF)

            rcopy(YS.at[ch, half], YV.at[ch, half], ys, yx.at[ch, half], (yp, ym)[half]).start()

    def count_send(step):
        dev = (bx1, bx2, by1, by2)[step]
        rcopy(CN.at[0, step], CN.at[1, step], cs, cx.at[step], dev).start()

    def count_wait(step):
        dev = (bx1, bx2, by1, by2)[step]
        rcopy(CN.at[1, step], CN.at[1, step], cs, cx.at[step], dev).wait_recv()
        return CN[0, step] + CN[1, step]

    rcopy(M.at[z, oc], M.at[z, oc], mps, mrx, mate).wait_recv()
    for side in range(2):
        msend(z, side, 1, True)

    ready(0)


    def blocks(i, hop):
        if hop == 0:
            process((i, 0, z))
        elif hop == 4:
            process((i, 7, away(4, 1)))
        else:
            both_sides(i, hop)

    def along_z(i, hop):
        if hop == 0:
            z0(i)
        elif hop == 4:
            z4(i)
        else:
            zhop(i, hop)

    def count_step(k):
        if k == 0:
            total = jnp.zeros((EXPERTS, TOK), F32)
            for zz in range(8):
                for cc in range(2):
                    total += jnp.where(M[zz, cc, 0:8, :] >= 0.0, 1.0, 0.0)
            CN[0, 0] = total
        else:
            CN[0, k] = count_wait(k - 1)
        count_send(k)

    def hidden_here():
        pltpu.make_async_copy(HB.at[:, c], HB.at[:, c], hsem).wait()
        rcopy(HB.at[:, oc], HB.at[:, oc], hps, hrx, mate).wait_recv()

    def multiply_last(ch):
        multiply_rest(ch)
        reduce_send(ch)

    acts = dict(
        r=ready, z=along_z, p=blocks, c=count_step, h=hidden_here, f=multiply_first,
        l=multiply_last,
    )
    for step in PLAN:
        acts[step[0]](*map(int, step[1:]))

    multiply_first(3)
    total = count_wait(3)
    picked = jnp.where(er == 2 * x + h, total, 0.0)
    count = jnp.sum(jnp.sum(picked, axis=1, keepdims=True), axis=0, keepdims=True)
    factor = lax.rsqrt(1.0 + count)
    arrive(3, 1)
    turn(3, 5, 7)
    for half in range(2):
        ywait(1, half)

    def groups(part, cols):
        return YV[part + 1, 0, :, cols].astype(F32) + YV[part + 1, 1, :, cols].astype(F32)

    @column_tiles
    def _(cols):
        ACC[:, cols] += partial(5, 7, cols)
        ACC[:HALF, cols] += groups(0, cols)

    arrive(3, 2)
    turn(3, 7, 8)
    for half in range(2):
        ywait(2, half)

    @column_tiles
    def _(cols):
        last = ACC[:, cols] + partial(7, 8, cols)
        out_ref[:HALF, cols] = last[:HALF] * factor
        out_ref[HALF:, cols] = (last[HALF:] + groups(1, cols)) * factor

    rcopy(M.at[z, c], M.at[z, c], mps, mrx, mate).wait_send()
    sent = Z.at[:, 0, pl.ds(0, TOK)]
    rcopy(sent, sent, psem, prx.at[0], mate).wait_send()
    rcopy(HB.at[:, c], HB.at[:, c], hps, hrx, mate).wait_send()
    sent = M.at[pl.ds(0, 7)]
    rcopy(sent, sent, ms, mx.at[0, 0], zp).wait_send()
    sent = Z.at[:, pl.ds(0, 7)]
    rcopy(sent, sent, zs, zx.at[0, 0, 0], zp).wait_send()
    rcopy(S, S, xs, rx.at[0, 0, 0], xp).wait_send()
    rcopy(YS, YS, ys, yx.at[0, 0], yp).wait_send()
    rcopy(CN.at[0], CN.at[0], cs, cx.at[0], bx1).wait_send()


def on_device(d_out, routes, combine, live_tokens, hidden):
    dma = pltpu.SemaphoreType.DMA
    any_spec = pl.BlockSpec(memory_space=pl.ANY)
    vmem = pl.BlockSpec(memory_space=pltpu.VMEM)
    return pl.pallas_call(
        kernel,
        out_shape=jax.ShapeDtypeStruct((WIDE, 1792), F32),
        in_specs=[any_spec, vmem, vmem, vmem, any_spec],
        out_specs=vmem,
        scratch_shapes=[
            pltpu.VMEM((CHUNKS, 8, 2 * TOK, WIDE), BF),
            pltpu.VMEM((CHUNKS, 8, 2, 4, CAP, WIDE), BF),
            pltpu.VMEM((CHUNKS, 8, 3, 2, CAP, WIDE), BF),
            pltpu.VMEM((8, 2, 4, CAP, 1792), BF),
            pltpu.VMEM((8, 2, 4 * CAP, TOK), BF),
            pltpu.VMEM((8, 2, 4 * CAP, TOK), F32),
            pltpu.VMEM((8, 2, 16, TOK), F32),
            pltpu.VMEM((2, 4, EXPERTS, TOK), F32),
            pltpu.VMEM((WIDE, 2 * 1536), BF),
            pltpu.VMEM((WIDE, 1792), F32),
            pltpu.VMEM((3, 2, HALF, 1792), BF),
            pltpu.VMEM((3, 2, HALF, 1792), BF),
            dma((CHUNKS,)), dma, dma((CHUNKS,)), dma, dma, dma, dma, dma,
            dma, dma((CHUNKS, 2, 4)), dma, dma((2, 4)),
            dma, dma((CHUNKS, 3, 3)),
            dma, dma((3, 2)), dma, dma((4,)),
        ],
        compiler_params=pltpu.CompilerParams(
            collective_id=0, has_side_effects=True, vmem_limit_bytes=54000000
        ),
    )(d_out, routes.T, combine.T, live_tokens.reshape(1, 1), hidden.reshape(4, 8, CAP, 1792))


def solution(mesh):
    both = P(("grp", "ep"), None)
    return jax.shard_map(
        on_device, mesh=mesh,
        in_specs=(both, both, both, P(("grp", "ep")), P("grp", "ep")),
        out_specs=P("grp", "ep"), check_vma=False,
    )
```
